128 devices in a mesh: blk: 16 (over y_lo, x, core), group: 8 (over z, y_hi).
Axes of the slice: x: 4, y: 4 (y_hi: 2, y_lo: 2; y = y_hi * 2 + y_lo), z: 4, core: 2. Of those that a mesh axis runs over, the one named last changes fastest.
Arguments:
- image_embed: bfloat16 [8192, 1152], P(('blk', 'group')), may hold values from -6 to 6
- caption_vectors: bfloat16 [65536, 1152], P(('blk', 'group')), may hold values from -6 to 6
- caption_counts: int32 [8192], replicated, may hold values from 1 to 8, as said below
- natural_log_multiplier: float32 [1], replicated, may hold values from 1.5 to 2.5
- match_odds_offset: float32 [1], replicated, may hold values from -6 to -4
Outputs:
- image_grad: float32 [8192, 1152], P(('blk', 'group'))
- caption_grad: float32 [65536, 1152], P(('blk', 'group'))
The draws below stay inside these ranges and needn't reach their ends.
Inputs may be any that keep to these rules, and one draw needn't show every extreme that they name: Images are numbered as in caption_counts, 64 to a device, devices in the order of blk then group. Local image k of the device with blk index b < 8 and group index g and local image k of the device with blk index b + 8 and group index g have counts that sum to 9. On at least one device all 64 images have 8 captions.
All inputs are finite; a program needn't handle non-finite values.
Results may differ from the reference program's by a relative error of at most 0.0028.
Values may be sent and summed in bfloat16 or wider, within the bound.
A program may use at most 64 MiB of HBM per device.

```python
import jax
import jax.numpy as jnp
from jax import lax

EMBED_WIDTH = 1152
NI_DEV = 64
CAP = 512
NI = 8192
CAPTION_SLOTS = 65536
N_BLK = 16
N_GROUP = 8
DEVICES = 128


def draw_caption_counts(key, part):
    half_blocks = N_BLK // 2
    level_key = jax.random.fold_in(key, 11)
    jitter_key = jax.random.fold_in(key, 12)
    flip_key = jax.random.fold_in(key, 13)
    full_key = jax.random.fold_in(key, 14)
    pair_level = jax.random.randint(level_key, (half_blocks, N_GROUP, 1), 1, 9)
    jitter = jax.random.randint(jitter_key, (half_blocks, N_GROUP, NI_DEV), -1, 2)
    lower_counts = jnp.clip(pair_level + jitter, 1, 8)
    full_pair = jax.random.randint(full_key, (), 0, half_blocks * N_GROUP)
    pair_number = jnp.arange(half_blocks * N_GROUP, dtype=jnp.int32).reshape(half_blocks, N_GROUP, 1)
    lower_counts = jnp.where(pair_number == full_pair, 8, lower_counts)
    flipped = jax.random.randint(flip_key, (half_blocks, N_GROUP, 1), 0, 2)
    lower_counts = jnp.where(flipped == 1, 9 - lower_counts, lower_counts)
    upper_counts = 9 - lower_counts
    return jnp.concatenate([lower_counts, upper_counts], axis=0).reshape(-1).astype(jnp.int32)


def centre_table(key):
    raw_centres = jax.random.normal(jax.random.fold_in(key, 21), (128, EMBED_WIDTH), jnp.float32)
    return raw_centres / jnp.sqrt(jnp.sum(raw_centres * raw_centres, axis=1, keepdims=True))


def image_clusters(key):
    return jax.random.randint(jax.random.fold_in(key, 22), (NI,), 0, 128).astype(jnp.int32)


def mixed_rows(base_key, salt, clusters, mix_low, mix_high, scale_low, scale_high):
    row_count = clusters.shape[0]
    row_key = jax.random.fold_in(base_key, salt)
    jitter_rows = jax.random.normal(jax.random.fold_in(row_key, 1), (row_count, EMBED_WIDTH), jnp.float32)
    jitter_rows = jitter_rows / jnp.sqrt(jnp.sum(jitter_rows * jitter_rows, axis=1, keepdims=True))
    mix_weight = jax.random.uniform(jax.random.fold_in(row_key, 2), (row_count, 1), jnp.float32, mix_low, mix_high)
    log_scale = jax.random.uniform(jax.random.fold_in(row_key, 3), (row_count, 1), jnp.float32, jnp.log(scale_low), jnp.log(scale_high))
    picked = jnp.take(centre_table(base_key), clusters, axis=0)
    return jnp.exp(log_scale) * (mix_weight * picked + jnp.sqrt(1.0 - mix_weight * mix_weight) * jitter_rows)


def draw_image_embed(key, part):
    clusters = image_clusters(key)
    values = mixed_rows(key, 23, clusters, 0.35, 0.85, 0.999, 1.001)
    return values.astype(jnp.bfloat16)


def draw_caption_vectors(key, part):
    counts = draw_caption_counts(key, part)
    per_device = counts.reshape(DEVICES, NI_DEV).astype(jnp.int32)
    running_end = jnp.cumsum(per_device, axis=1).astype(jnp.int32)
    position = jnp.arange(CAP, dtype=jnp.int32)
    local_index = jnp.sum((running_end[:, None, :] <= position[None, :, None]).astype(jnp.int32), axis=2).astype(jnp.int32)
    first_image = (jnp.arange(DEVICES, dtype=jnp.int32) * NI_DEV)[:, None]
    live_slots = position[None, :] < running_end[:, -1:]
    owners = jnp.where(live_slots, first_image + local_index, 0).reshape(-1).astype(jnp.int32)
    owner_clusters = jnp.take(image_clusters(key), owners)
    spare_clusters = jax.random.randint(jax.random.fold_in(key, 24), (CAPTION_SLOTS,), 0, 128).astype(jnp.int32)
    clusters = jnp.where(live_slots.reshape(-1), owner_clusters, spare_clusters).astype(jnp.int32)
    values = mixed_rows(key, 25, clusters, 0.35, 0.85, 0.999, 1.001)
    return values.astype(jnp.bfloat16)


def setup_inputs(seed: int = 0) -> dict:
    streams_of = jax.random.split(jax.random.key(seed), 6)
    image_embed = draw_image_embed(jax.random.fold_in(streams_of[5], 71), 0)
    caption_vectors = draw_caption_vectors(jax.random.fold_in(streams_of[5], 71), 0)
    caption_counts = draw_caption_counts(jax.random.fold_in(streams_of[5], 71), 0)
    natural_log_multiplier = jnp.clip(jax.random.uniform(streams_of[3], (1,), jnp.float32, 1.5, 2.5), 1.5, 2.5)
    match_odds_offset = jnp.clip(jax.random.uniform(streams_of[4], (1,), jnp.float32, -6.0, -4.0), -6.0, -4.0)
    return dict(image_embed=image_embed, caption_vectors=caption_vectors, caption_counts=caption_counts, natural_log_multiplier=natural_log_multiplier, match_odds_offset=match_odds_offset)


EPSILON = 1e-06

def normalize(embed_rows):
    values = embed_rows.astype(jnp.float32)
    inverse = lax.rsqrt(lax.optimization_barrier(jnp.sum(values * values, axis=1, keepdims=True)) + EPSILON)
    return (values * inverse, inverse)

def owner_table(caption_counts):
    per_device = caption_counts.reshape(DEVICES, NI_DEV).astype(jnp.int32)
    running_end = jnp.cumsum(per_device, axis=1).astype(jnp.int32)
    position = jnp.arange(CAP, dtype=jnp.int32)
    local_index = lax.optimization_barrier(jnp.sum((running_end[:, None, :] <= position[None, :, None]).astype(jnp.int32), axis=2)).astype(jnp.int32)
    first_image = (jnp.arange(DEVICES, dtype=jnp.int32) * NI_DEV)[:, None]
    present_entry_flags = position[None, :] < running_end[:, -1:]
    return jnp.where(present_entry_flags, first_image + local_index, -1).astype(jnp.int32)

def reference(image_embed, caption_vectors, caption_counts, natural_log_multiplier, match_odds_offset):
    image_unit, image_inverse = normalize(image_embed)
    caption_unit, caption_inverse = normalize(caption_vectors)
    image_low = image_unit.astype(jnp.bfloat16)
    caption_low = caption_unit.astype(jnp.bfloat16)
    owners = owner_table(caption_counts)
    odds_sharpness_factor = jnp.exp(natural_log_multiplier[0])
    image_ids = jnp.arange(NI, dtype=jnp.int32)
    picture_entry_extent = image_low.T

    def one_block(image_sum, inputs):
        tile_line_extent, block_owner = inputs
        similarity_matrix = odds_sharpness_factor * jnp.dot(tile_line_extent, picture_entry_extent, preferred_element_type=jnp.float32) + match_odds_offset[0]
        match_target_signs = jnp.where(block_owner[:, None] == image_ids[None, :], 1.0, -1.0)
        present_entry_flags = (block_owner >= 0)[:, None]
        oriented_similarity_gap = match_target_signs * similarity_matrix
        match_loss_factors = jnp.where(present_entry_flags, odds_sharpness_factor * (-match_target_signs * jax.nn.sigmoid(-oriented_similarity_gap)), 0.0).astype(jnp.bfloat16)
        caption_sum = jnp.dot(match_loss_factors, image_low, preferred_element_type=jnp.float32)
        image_sum = image_sum + jnp.dot(match_loss_factors.T, tile_line_extent, preferred_element_type=jnp.float32)
        return (image_sum, caption_sum)
    initial = jnp.zeros((NI, EMBED_WIDTH), jnp.float32)
    image_sum, caption_sum = lax.scan(one_block, initial, (caption_low.reshape(DEVICES, CAP, EMBED_WIDTH), owners))
    caption_sum = caption_sum.reshape(DEVICES * CAP, EMBED_WIDTH)
    image_grad = (image_sum - image_unit * lax.optimization_barrier(jnp.sum(image_unit * image_sum, axis=1, keepdims=True))) * image_inverse
    slot_live = (owners.reshape(-1) >= 0)[:, None]
    caption_grad = jnp.where(slot_live, (caption_sum - caption_unit * lax.optimization_barrier(jnp.sum(caption_unit * caption_sum, axis=1, keepdims=True))) * caption_inverse, 0.0)
    return (image_grad, caption_grad)
```

```python
import jax
import jax.numpy as jnp
from jax import lax
from jax.experimental import pallas as pl
from jax.experimental.pallas import tpu as pltpu
from jax.sharding import PartitionSpec as P

EPSILON = 1e-06
R = 32
F32 = jnp.float32
BF16 = jnp.bfloat16


def normalize(rows):
    values = rows.astype(F32)
    inverse = lax.rsqrt(jnp.sum(values * values, axis=1, keepdims=True) + EPSILON)
    return values * inverse, inverse


class Copies:
    def __init__(self, send_sem, recv_sem):
        self.send_sem, self.recv_sem, self.named = send_sem, recv_sem, {}

    def send(self, name, src, dst, device):
        index = len(self.named)
        copy = pltpu.make_async_remote_copy(
            src_ref=src,
            dst_ref=dst,
            send_sem=self.send_sem.at[index],
            recv_sem=self.recv_sem.at[index],
            device_id=device,
            device_id_type=pl.DeviceIdType.MESH,
        )
        copy.start()
        self.named[name] = copy

    def wait(self, *name):
        self.named[name].wait_recv()

    def drain(self):
        for copy in self.named.values():
            copy.wait_send()


def kernel(
    img_ref, cap_ref, cnt_ref, nlm_ref, bias_ref, iout, cout,
    imgbuf, capbuf, head, tsend, trecv, wt, midx, tots, consts,
    pown, d2ds, d2dr, zsrel, zsdir, zsdep, zrrel, zrdir, zrdep, gs, gsb, ts2, tr2,
    xown, xdep, xsrel, xsdir, xsdep, xrrel, xrdir, xrdep,
    yown, ydep, ysrel, ysdir, ysdep, yrrel, yrdir, yrdep,
    send_sem, recv_sem,
):
    n_img, width = img_ref.shape
    n_slot = cap_ref.shape[0]
    kept = 9 * n_img // 2
    nk = kept // R
    nt = (n_slot - kept) // R
    cols = 4 * n_img
    rows = 8 * R
    half = n_img // 2
    blk = lax.axis_index("blk")
    grp = lax.axis_index("group")
    core, x, ylo = lax.rem(blk, 2), lax.rem(lax.div(blk, 2), 4), lax.div(blk, 8)
    z, yhi = lax.div(grp, 2), lax.rem(grp, 2)
    y = yhi * 2 + ylo

    def dev(dx=0, dy=0, dz=0):
        px, py, pz = lax.rem(x + dx + 4, 4), lax.rem(y + dy + 4, 4), lax.rem(z + dz + 4, 4)
        return ((lax.rem(py, 2) * 4 + px) * 2 + core, pz * 2 + lax.div(py, 2))

    sibling = (blk + 1 - 2 * core, grp)
    partner = (((1 - ylo) * 4 + x) * 2 + core, grp)
    copies = Copies(send_sem, recv_sem)

    barrier = pltpu.get_barrier_semaphore()
    for device in (dev(1), dev(-1), dev(0, 1), dev(0, -1), dev(0, 0, 1), dev(0, 0, -1), sibling):
        pl.semaphore_signal(barrier, inc=1, device_id=device, device_id_type=pl.DeviceIdType.MESH)
    pl.semaphore_wait(barrier, 7)

    def img_at(xr, yr, first=0, count=n_img):
        return imgbuf.at[pl.ds(xr * cols + yr * n_img + first, count)]

    def cap_at(k, core_rel, zr):
        return capbuf.at[pl.ds(k * rows + core_rel * 4 * R + zr * R, R)]

    def send_x(yr):
        copies.send(("xp", yr), img_at(0, yr), img_at(1, yr), dev(1))
        copies.send(("xm", yr), img_at(0, yr), img_at(3, yr), dev(-1))

    def relay_x(yr):
        copies.wait("xp", yr)
        copies.wait("xm", yr)
        if yr % 2 == 0:
            copies.send(("xr", yr), img_at(1, yr), img_at(2, yr), dev(1))
        else:
            copies.send(("xr", yr), img_at(3, yr), img_at(2, yr), dev(-1))

    imgbuf[pl.ds(0, n_img), :] = normalize(img_ref[...])[0].astype(BF16)
    send_x(0)

    def send_tail(t):
        tsend[t] = normalize(cap_ref[pl.ds(kept + t * R, R), :])[0].astype(BF16)
        copies.send(("t", t), tsend.at[t], trecv.at[pl.ds(t * R, R)], partner)

    send_tail(0)
    copies.send(("yp",), img_at(0, 0), img_at(0, 1), dev(0, 1))
    copies.send(("ym",), img_at(0, 0), img_at(0, 3), dev(0, -1))

    lower = (
        lax.broadcasted_iota(jnp.int32, (n_img, n_img), 0)
        >= lax.broadcasted_iota(jnp.int32, (n_img, n_img), 1)
    ).astype(F32)

    def running_ends(device, lanes):
        counts = cnt_ref[pl.ds(device[0] * 8 + device[1], 1), :].astype(F32)
        return jnp.dot((lower * counts).astype(BF16), jnp.ones((n_img, lanes), BF16), preferred_element_type=F32)

    own_ends = running_ends((blk, grp), width)
    tots[0:1, :] = own_ends[n_img - 1 :, :]
    log_row = jnp.full((1, rows), nlm_ref[0], F32)
    consts[0:1, :] = jnp.exp(log_row) * 0.5
    consts[1:2, :] = jnp.full((1, rows), bias_ref[0] * 0.5, F32)

    def before_total(first):
        position = lax.broadcasted_iota(jnp.int32, (R, width), 0) + first
        return position.astype(F32) < tots[0:1, :]

    def pack(k):
        block = normalize(cap_ref[pl.ds(k * R, R), :])[0]
        if k >= 2:
            count = (k - 1) * R
            row = (lax.broadcasted_iota(jnp.int32, (R, count), 0) + k * R).astype(F32)
            lane = lax.broadcasted_iota(jnp.int32, (R, count), 1).astype(F32)
            pick = jnp.where(row - tots[0:1, :count] == lane, 1.0, 0.0).astype(BF16)
            moved = jnp.dot(pick, trecv[pl.ds(0, count), :], preferred_element_type=F32)
            block = jnp.where(before_total(k * R), block, moved)
        capbuf[pl.ds(k * rows, R), :] = block.astype(BF16)
        copies.send(("zp", k), cap_at(k, 0, 0), cap_at(k, 0, 1), dev(0, 0, 1))
        copies.send(("zm", k), cap_at(k, 0, 0), cap_at(k, 0, 3), dev(0, 0, -1))
        copies.send(("s0", k), cap_at(k, 0, 0), cap_at(k, 1, 0), sibling)

    pack(0)
    pack(1)
    for t in range(1, nt):
        send_tail(t)

    own_part = own_ends[:, :rows]
    pair_ends = running_ends(partner, rows)
    pair_first = ((3 - 2 * ylo) * n_img).astype(F32)
    total_row = own_part[n_img - 1 :, :]
    lane = lax.broadcasted_iota(jnp.int32, (1, rows), 1)
    for k in range(nk):
        position = (lane + k * R).astype(F32)
        own_index = jnp.sum(jnp.where(own_part <= position, 1.0, 0.0), axis=0, keepdims=True)
        slot = position - total_row + float(kept)
        pair_index = jnp.sum(jnp.where(pair_ends <= slot, 1.0, 0.0), axis=0, keepdims=True)
        column = jnp.where(position < total_row, own_index, pair_first + pair_index)
        midx[k : k + 1, :] = jnp.where(lane < R, column, -1.0).astype(jnp.int32)

    def weights(k, xr, match):
        first_img = pl.multiple_of(xr * cols, cols)
        first_cap = pl.multiple_of(k * rows, rows)
        products = lax.dot_general(
            imgbuf[pl.ds(first_img, cols), :],
            capbuf[pl.ds(first_cap, rows), :],
            (((1,), (1,)), ((), ())),
            preferred_element_type=F32,
        )
        scale = consts[0:1, :]
        half_tanh = scale * jnp.tanh(products * scale + consts[1:2, :])
        if match:
            image = lax.broadcasted_iota(jnp.int32, (cols, rows), 0)
            half_tanh = half_tanh + jnp.where(image == midx[k : k + 1, :], -scale, scale)
        else:
            half_tanh = half_tanh + scale
        wt[pl.ds(first_img, cols), pl.ds(first_cap, rows)] = half_tanh.astype(BF16)

    def weights_of(xr, first, last):
        @pl.loop(first, last)
        def _(k):
            weights(k, xr, False)

    def forward(kind, k, zr):
        copies.send((kind, k), cap_at(k, 0, zr), cap_at(k, 1, zr), sibling)

    def chunk_in(k):
        for kind in ("s0", "s1", "s2", "s3"):
            copies.wait(kind, k)
        weights(k, 0, True)

    for j in range(nk):
        if j + 2 < nk:
            copies.wait("t", j)
            pack(j + 2)
        if j == 0:
            copies.wait("yp")
            copies.wait("ym")
            copies.send(("yr", 0), img_at(0, 1, 0, half), img_at(0, 2, 0, half), dev(0, 1))
            copies.send(("yr", 1), img_at(0, 3, half, half), img_at(0, 2, half, half), dev(0, -1))
            send_x(1)
            send_x(3)
        if j == 1:
            relay_x(0)
        copies.wait("zp", j)
        copies.wait("zm", j)
        if j % 2 == 0:
            copies.send(("zr", j), cap_at(j, 0, 1), cap_at(j, 0, 2), dev(0, 0, 1))
        else:
            copies.send(("zr", j), cap_at(j, 0, 3), cap_at(j, 0, 2), dev(0, 0, -1))
        forward("s1", j, 1)
        forward("s3", j, 3)
        if j == 2:
            copies.wait("yr", 0)
            copies.wait("yr", 1)
            send_x(2)
        if j >= 1:
            copies.wait("zr", j - 1)
            forward("s2", j - 1, 2)
        if j == 3:
            relay_x(1)
        if j == 5:
            relay_x(3)
        if j == 6:
            relay_x(2)
        if j >= 3:
            chunk_in(j - 3)
        if j == 7:
            weights_of(1, 0, 5)
        if j == 8:
            weights_of(3, 0, 5)
    copies.wait("zr", nk - 1)
    forward("s2", nk - 1, 2)
    for k in range(nk - 3, nk):
        chunk_in(k)
    weights_of(1, 5, nk)
    weights_of(3, 5, nk)
    for yr in (0, 1, 3, 2):
        copies.wait("xr", yr)
    weights_of(2, 0, nk)

    def caption_part(k):
        part = lax.dot_general(
            wt[:, pl.ds(k * rows, rows)], imgbuf[...], (((0,), (0,)), ((), ())), preferred_element_type=F32
        )
        pown[k] = part[: 4 * R, :]
        d2ds[k] = part[4 * R :, :].astype(BF16)
        copies.send(("d", k), d2ds.at[k], d2dr.at[k], sibling)

    def image_part(xr):
        return jnp.dot(wt[pl.ds(xr * cols, cols), :], capbuf[...], preferred_element_type=F32)

    def sign(index):
        return 1 if index % 2 == 0 else -1

    def z_first(k):
        copies.wait("d", k)
        step = sign(k)
        direct, late = (1, 3) if step == 1 else (3, 1)

        def total(zr):
            here = slice(zr * R, zr * R + R)
            return pown[k, here, :] + d2dr[k, here, :].astype(F32)

        zsrel[k] = total(2).astype(BF16)
        copies.send(("zrel", k), zsrel.at[k], zrrel.at[k], dev(0, 0, step))
        zsdir[k] = total(direct).astype(BF16)
        copies.send(("zdir", k), zsdir.at[k], zrdir.at[k], dev(0, 0, -step))
        pown[k, 0:R, :] = total(0)
        pown[k, late * R : late * R + R, :] = total(late)

    def z_late(k):
        copies.wait("zrel", k)
        step = sign(k)
        late = 3 if step == 1 else 1
        zsdep[k] = (pown[k, late * R : late * R + R, :] + zrrel[k].astype(F32)).astype(BF16)
        copies.send(("zdep", k), zsdep.at[k], zrdep.at[k], dev(0, 0, step))

    def project(first, sums, live):
        unit, inverse = normalize(cap_ref[pl.ds(first, R), :])
        grads = (sums - unit * jnp.sum(unit * sums, axis=1, keepdims=True)) * inverse
        cout[pl.ds(first, R), :] = jnp.where(live, grads, 0.0)

    def z_last(k):
        copies.wait("zdir", k)
        copies.wait("zdep", k)
        sums = pown[k, 0:R, :] + zrdir[k].astype(F32) + zrdep[k].astype(F32)
        gsb[pl.ds(k * R, R), :] = sums.astype(BF16)
        if k >= 2:
            t = k - 2
            count = kept - k * R
            row = lax.broadcasted_iota(jnp.int32, (R, count), 0).astype(F32)
            lane = (lax.broadcasted_iota(jnp.int32, (R, count), 1) + 2 * R).astype(F32)
            pick = jnp.where(row + tots[0:1, :count] == lane, 1.0, 0.0).astype(BF16)
            ts2[t] = jnp.dot(pick, gsb[pl.ds(k * R, count), :], preferred_element_type=F32).astype(BF16)
            copies.send(("tb", t), ts2.at[t], tr2.at[t], partner)
        live = before_total(k * R)
        project(k * R, jnp.where(live, sums, 0.0), live)

    def tail_last(t):
        copies.wait("tb", t)
        live = before_total(kept + t * R)
        project(kept + t * R, jnp.where(live, tr2[t].astype(F32), 0.0), live)

    def x_first(xr):
        part = image_part(xr)
        if xr == 0:
            xown[...] = part
            return
        if xr == 2:
            xsrel[...] = part.astype(BF16)
            for yr in (2, 1, 3, 0):
                here = pl.ds(yr * n_img, n_img)
                copies.send(("xrel", yr), xsrel.at[here], xrrel.at[here], dev(sign(yr)))
            return
        for yr in (2, 0, 1, 3):
            here = pl.ds(yr * n_img, n_img)
            piece = part[yr * n_img : (yr + 1) * n_img, :]
            if (sign(yr) == 1) == (xr == 3):
                xdep[here, :] = piece
            else:
                xsdir[here, :] = piece.astype(BF16)
                copies.send(("xdir", yr), xsdir.at[here], xrdir.at[here], dev(-sign(yr)))

    def x_late(yr):
        copies.wait("xrel", yr)
        here = pl.ds(yr * n_img, n_img)
        xsdep[here, :] = (xdep[here, :] + xrrel[here, :].astype(F32)).astype(BF16)
        copies.send(("xdep", yr), xsdep.at[here], xrdep.at[here], dev(sign(yr)))

    low, high = pl.ds(0, half), pl.ds(half, half)

    def x_last(yr):
        copies.wait("xdir", yr)
        copies.wait("xdep", yr)
        here = pl.ds(yr * n_img, n_img)
        sums = xown[here, :] + xrdir[here, :].astype(F32) + xrdep[here, :].astype(F32)
        if yr == 0:
            yown[...] = sums
        elif yr == 2:
            ysrel[...] = sums.astype(BF16)
            copies.send(("yrel", 0), ysrel.at[low], yrrel.at[low], dev(0, 1))
            copies.send(("yrel", 1), ysrel.at[high], yrrel.at[high], dev(0, -1))
        elif yr == 1:
            ysdir[low, :] = sums[:half, :].astype(BF16)
            copies.send(("ydir", 0), ysdir.at[low], yrdir.at[low], dev(0, -1))
            ydep[high, :] = sums[half:, :]
        else:
            ysdir[high, :] = sums[half:, :].astype(BF16)
            copies.send(("ydir", 1), ysdir.at[high], yrdir.at[high], dev(0, 1))
            ydep[low, :] = sums[:half, :]

    def y_late(part):
        copies.wait("yrel", part)
        here = (low, high)[part]
        ysdep[here, :] = (ydep[here, :] + yrrel[here, :].astype(F32)).astype(BF16)
        copies.send(("ydep", part), ysdep.at[here], yrdep.at[here], dev(0, (1, -1)[part]))

    caption_part(8)
    x_first(2)
    z_first(8)
    caption_part(7)
    x_first(1)
    z_first(7)
    caption_part(6)
    x_first(3)
    z_first(6)
    caption_part(5)
    z_late(8)
    x_first(0)
    z_first(5)
    caption_part(4)
    z_late(7)
    for k in (3, 2, 1, 0):
        z_first(k + 1)
        caption_part(k)
        z_late(k + 3)
    z_first(0)
    x_late(2)
    z_last(8)
    z_late(2)
    x_late(1)
    z_last(7)
    x_late(3)
    z_late(1)
    z_last(6)
    x_late(0)
    z_late(0)
    z_last(5)
    z_last(4)
    x_last(2)
    z_last(3)
    x_last(1)
    x_last(3)
    y_late(0)
    y_late(1)
    z_last(2)
    x_last(0)
    z_last(1)
    z_last(0)
    for t in reversed(range(nt)):
        tail_last(t)
    for name in (("ydir", 0), ("ydir", 1), ("ydep", 0), ("ydep", 1)):
        copies.wait(*name)
    sums = yown[...] + yrdir[...].astype(F32) + yrdep[...].astype(F32)
    unit, inverse = normalize(img_ref[...])
    iout[...] = (sums - unit * jnp.sum(unit * sums, axis=1, keepdims=True)) * inverse
    copies.drain()


def shards(image_embed, caption_vectors, caption_counts, natural_log_multiplier, match_odds_offset):
    n_img, width = image_embed.shape
    n_slot = caption_vectors.shape[0]
    kept = 9 * n_img // 2
    nk, nt = kept // R, (n_slot - kept) // R
    cols, rows = 4 * n_img, 8 * R
    vmem = pl.BlockSpec(memory_space=pltpu.VMEM)
    smem = pl.BlockSpec(memory_space=pltpu.SMEM)

    def buf(*shape, dtype=BF16):
        return pltpu.VMEM((*shape, width), dtype)

    scratch = [
        buf(4 * cols),
        buf(nk * rows),
        buf(R),
        buf(nt, R),
        buf(nt * R),
        pltpu.VMEM((4 * cols, nk * rows), BF16),
        pltpu.VMEM((16, rows), jnp.int32),
        pltpu.VMEM((8, width), F32),
        pltpu.VMEM((8, rows), F32),
        buf(nk, 4 * R, dtype=F32),
        buf(nk, 4 * R),
        buf(nk, 4 * R),
        *[buf(nk, R)] * 6,
        buf(R, dtype=F32),
        buf(kept),
        buf(nt, R),
        buf(nt, R),
        *[buf(cols, dtype=F32)] * 2,
        *[buf(cols)] * 6,
        *[buf(n_img, dtype=F32)] * 2,
        *[buf(n_img)] * 6,
        pltpu.SemaphoreType.DMA((160,)),
        pltpu.SemaphoreType.DMA((160,)),
    ]
    return pl.pallas_call(
        kernel,
        out_shape=(
            jax.ShapeDtypeStruct((n_img, width), F32),
            jax.ShapeDtypeStruct((n_slot, width), F32),
        ),
        in_specs=[vmem, vmem, vmem, smem, smem],
        out_specs=(vmem, vmem),
        scratch_shapes=scratch,
        compiler_params=pltpu.CompilerParams(
            collective_id=0, has_side_effects=True, vmem_limit_bytes=60 * 1024 * 1024
        ),
    )(image_embed, caption_vectors, caption_counts.reshape(-1, n_img), natural_log_multiplier, match_odds_offset)


def solution(mesh):
    placed = (P(("blk", "group"), None), P(("blk", "group"), None), P(), P(), P())
    return jax.shard_map(
        shards,
        mesh=mesh,
        in_specs=placed,
        out_specs=(P(("blk", "group"), None), P(("blk", "group"), None)),
        check_vma=False,
    )
```

```python
import jax
import jax.numpy as jnp
from jax import lax
from jax.experimental import pallas as pl
from jax.experimental.pallas import tpu as pltpu
from jax.sharding import PartitionSpec as P

EPSILON = 1e-06
R = 32
F32 = jnp.float32
BF16 = jnp.bfloat16


YPOS = 2
ORDER = (
    ("sx", 0), ("t", 0), ("t", 1), ("p", 0), ("p", 1), ("t", 2), ("t", 3), ("t", 4), ("t", 5), ("t", 6), ("p", 2),
    ("f", 0, 1), ("f", 0, 3), ("rx", 0), ("p", 3), ("ry", 3), ("sx", 3), ("f", 1, 3), ("f", 1, 1), ("f", 2, 1),
    ("f", 2, 3), ("ry", 1), ("sx", 1), ("f", 3, 3), ("f", 0, 2), ("p", 4), ("f", 1, 2), ("f", 3, 1), ("rx", 3),
    ("p", 5), ("f", 2, 2), ("f", 3, 2), ("p", 6), ("f", 4, 1), ("rx", 1), ("f", 4, 3), ("p", 7), ("f", 5, 1),
    ("f", 5, 3), ("p", 8), ("f", 6, 1), ("f", 6, 3), ("sx", 2), ("A", 0, 0), ("A", 1, 0), ("A", 2, 0), ("A", 3, 0),
    ("f", 4, 2), ("f", 7, 3), ("A", 4, 0), ("f", 7, 1), ("f", 5, 2), ("f", 8, 1), ("A", 5, 0), ("f", 8, 3), ("rx", 2),
    ("A", 5, 1), ("A", 1, 1), ("A", 2, 3), ("A", 2, 1), ("A", 4, 3), ("A", 0, 3), ("A", 3, 1), ("A", 3, 3),
    ("A", 1, 3), ("A", 5, 3), ("f", 6, 2), ("A", 0, 1), ("A", 4, 1), ("f", 7, 2), ("f", 8, 2), ("A", 6, 0),
    ("A", 6, 1), ("A", 6, 3), ("A", 7, 3), ("A", 8, 3), ("A", 7, 1), ("A", 8, 1), ("A", 7, 0), ("A", 8, 0),
    ("C", 1, 0), ("A", 8, 2), ("B", 8), ("A", 6, 2), ("A", 4, 2), ("A", 1, 2), ("A", 2, 2), ("A", 0, 2), ("A", 7, 2),
    ("B", 7), ("A", 3, 2), ("A", 5, 2), ("zf", 8), ("B", 6), ("C", 2, 0), ("zf", 7), ("B", 5), ("C", 0, 1), ("zf", 6),
    ("C", 2, 1), ("zl", 8), ("C", 0, 0), ("zf", 5), ("B", 4), ("zl", 7), ("B", 3), ("C", 3, 0), ("xl", 2), ("zl", 6),
    ("C", 3, 1), ("zf", 4), ("zz", 8), ("zf", 3), ("zl", 5), ("B", 2), ("B", 1), ("zz", 7), ("xl", 0), ("C", 1, 1),
    ("xl", 1), ("zz", 6), ("zf", 2), ("B", 0), ("e", 6), ("xl", 3), ("xz", 2), ("zl", 4), ("zl", 3), ("zf", 1),
    ("e", 5), ("zf", 0), ("zz", 5), ("e", 4), ("zl", 2), ("xz", 1), ("yz", 1), ("zz", 4), ("zz", 3), ("e", 3),
    ("xz", 3), ("zl", 1), ("yz", 0), ("zl", 0), ("xz", 0), ("zz", 2), ("e", 2), ("zz", 1), ("zz", 0), ("end",),
    ("e", 1), ("e", 0),
)


def normalize(rows):
    values = rows.astype(F32)
    inverse = lax.rsqrt(jnp.sum(values * values, axis=1, keepdims=True) + EPSILON)
    return values * inverse, inverse


class Copies:
    def __init__(self, send_sem, recv_sem):
        self.send_sem, self.recv_sem, self.named, self.open = send_sem, recv_sem, {}, set()

    def send(self, name, src, dst, device):
        index = len(self.named)
        copy = pltpu.make_async_remote_copy(
            src_ref=src,
            dst_ref=dst,
            send_sem=self.send_sem.at[index],
            recv_sem=self.recv_sem.at[index],
            device_id=device,
            device_id_type=pl.DeviceIdType.MESH,
        )
        copy.start()
        self.named[name] = copy
        self.open.add(name)

    def wait(self, *name):
        if name in self.open:
            self.named[name].wait_recv()
            self.open.remove(name)

    def drain(self):
        for name, copy in self.named.items():
            self.wait(*name)
            copy.wait_send()


def kernel(
    img_ref, cap_ref, cnt_ref, nlm_ref, bias_ref, iout, cout,
    imgbuf, capbuf, head, tsend, trecv, wt, midx, tots, consts,
    pown, d2ds, d2dr, zsrel, zsdir, zsdep, zrrel, zrdir, zrdep, gs, gsb, ts2, tr2,
    xown, xdep, xsrel, xsdir, xsdep, xrrel, xrdir, xrdep,
    yown, ydep, ysrel, ysdir, ysdep, yrrel, yrdir, yrdep,
    send_sem, recv_sem,
):
    n_img, width = img_ref.shape
    n_slot = cap_ref.shape[0]
    kept = 9 * n_img // 2
    nk = kept // R
    nt = (n_slot - kept) // R
    cols = 4 * n_img
    rows = 8 * R
    half = n_img // 2
    blk = lax.axis_index("blk")
    grp = lax.axis_index("group")
    core, x, ylo = lax.rem(blk, 2), lax.rem(lax.div(blk, 2), 4), lax.div(blk, 8)
    z, yhi = lax.div(grp, 2), lax.rem(grp, 2)
    y = yhi * 2 + ylo
    near = 1 - 2 * ylo

    def dev(dx=0, dy=0, dz=0):
        px, py, pz = lax.rem(x + dx + 4, 4), lax.rem(y + dy + 4, 4), lax.rem(z + dz + 4, 4)
        return ((lax.rem(py, 2) * 4 + px) * 2 + core, pz * 2 + lax.div(py, 2))

    sibling = (blk + 1 - 2 * core, grp)
    partner = (((1 - ylo) * 4 + x) * 2 + core, grp)
    copies = Copies(send_sem, recv_sem)

    barrier = pltpu.get_barrier_semaphore()
    for device in (dev(1), dev(-1), dev(0, 1), dev(0, -1), dev(0, 0, 1), dev(0, 0, -1), sibling):
        pl.semaphore_signal(barrier, inc=1, device_id=device, device_id_type=pl.DeviceIdType.MESH)

    place = (0, 2, 1, 3)

    def img_at(xr, yr, first=0, count=n_img):
        return imgbuf.at[pl.ds(xr * cols + place[yr] * n_img + first, count)]

    def cap_at(k, core_rel, zr):
        return capbuf.at[pl.ds(k * rows + core_rel * 4 * R + zr * R, R)]

    def sign(index):
        return 1 if index % 2 == 0 else -1

    imgbuf[pl.ds(0, n_img), :] = normalize(img_ref[...])[0].astype(BF16)
    for t in range(nt):
        tsend[t] = normalize(cap_ref[pl.ds(kept + t * R, R), :])[0].astype(BF16)

    two = 2 * n_img
    image_row = lax.broadcasted_iota(jnp.int32, (n_img, two), 0)
    image_lane = lax.broadcasted_iota(jnp.int32, (n_img, two), 1)

    def running_ends(device, lanes):
        number = device[0] * 8 + device[1]
        counts = cnt_ref[pl.ds(lax.div(number, 2), 1), :].astype(F32)
        local = image_lane - lax.rem(number, 2) * n_img
        lower = jnp.where(jnp.logical_and(local >= 0, local <= image_row), counts, 0.0)
        return jnp.dot(lower.astype(BF16), jnp.ones((two, lanes), BF16), preferred_element_type=F32)

    own_ends = running_ends((blk, grp), width)
    tots[0:1, :] = own_ends[n_img - 1 :, :]
    log_row = jnp.full((1, rows), nlm_ref[0], F32)
    consts[0:1, :] = jnp.exp(log_row) * 0.5
    consts[1:2, :] = jnp.full((1, rows), bias_ref[0] * 0.5, F32)

    own_part = own_ends[:, :rows]
    pair_ends = running_ends(partner, rows)
    total_row = own_part[n_img - 1 :, :]
    lane = lax.broadcasted_iota(jnp.int32, (1, rows), 1)
    for k in range(nk):
        position = (lane + k * R).astype(F32)
        own_index = jnp.sum(jnp.where(own_part <= position, 1.0, 0.0), axis=0, keepdims=True)
        slot = position - total_row + float(kept)
        pair_index = jnp.sum(jnp.where(pair_ends <= slot, 1.0, 0.0), axis=0, keepdims=True)
        column = jnp.where(position < total_row, own_index, float(place[1] * n_img) + pair_index)
        midx[k : k + 1, :] = jnp.where(lane < R, column, -1.0).astype(jnp.int32)

    pl.semaphore_wait(barrier, 7)

    def before_total(first):
        position = lax.broadcasted_iota(jnp.int32, (R, width), 0) + first
        return position.astype(F32) < tots[0:1, :]

    def send_x(yr):
        if yr == 2:
            copies.wait("y2", 1)
            copies.wait("y2", 3)
        elif yr:
            copies.wait("y", yr)
        copies.send(("xp", yr), img_at(0, yr), img_at(1, yr), dev(1))
        copies.send(("xm", yr), img_at(0, yr), img_at(3, yr), dev(-1))

    def relay_x(yr):
        kind, xr = ("xp", 1) if yr % 2 == 0 else ("xm", 3)
        copies.wait(kind, yr)
        copies.send(("xr", yr), img_at(xr, yr), img_at(2, yr), dev(sign(yr)))

    def relay_y(yr):
        copies.wait("y", yr)
        first, step = (0, -near) if yr == 1 else (half, near)
        copies.send(("y2", yr), img_at(0, yr, first, half), img_at(0, 2, first, half), dev(0, step))

    def tail(t):
        copies.send(("t", t), tsend.at[t], trecv.at[pl.ds(t * R, R)], partner)
        if t == YPOS - 1:
            copies.send(("y", 1), img_at(0, 0), img_at(0, 1), partner)
            copies.send(("y", 3), img_at(0, 0), img_at(0, 3), dev(0, -near))

    def pack(k):
        block = normalize(cap_ref[pl.ds(k * R, R), :])[0]
        if k >= 2:
            copies.wait("t", k - 2)
            count = (k - 1) * R
            row = (lax.broadcasted_iota(jnp.int32, (R, count), 0) + k * R).astype(F32)
            lane = lax.broadcasted_iota(jnp.int32, (R, count), 1).astype(F32)
            pick = jnp.where(row - tots[0:1, :count] == lane, 1.0, 0.0).astype(BF16)
            moved = jnp.dot(pick, trecv[pl.ds(0, count), :], preferred_element_type=F32)
            block = jnp.where(before_total(k * R), block, moved)
        capbuf[pl.ds(k * rows, R), :] = block.astype(BF16)
        copies.send(("zp", k), cap_at(k, 0, 0), cap_at(k, 0, 1), dev(0, 0, 1))
        copies.send(("zm", k), cap_at(k, 0, 0), cap_at(k, 0, 3), dev(0, 0, -1))
        copies.send(("s", 0, k), cap_at(k, 0, 0), cap_at(k, 1, 0), sibling)

    def forward(k, zr):
        copies.wait(("", "zp", "zr", "zm")[zr], k)
        if zr != 2 and (zr == 1) == (k % 2 == 0):
            copies.send(("zr", k), cap_at(k, 0, zr), cap_at(k, 0, 2), dev(0, 0, sign(k)))
        copies.send(("s", zr, k), cap_at(k, 0, zr), cap_at(k, 1, zr), sibling)

    def weights(k, xr):
        for zr in range(4):
            copies.wait("s", zr, k)
        if xr == 0:
            for name in (("y", 1), ("y", 3), ("y2", 1), ("y2", 3)):
                copies.wait(*name)
        else:
            for yr in range(4):
                copies.wait(("", "xp", "xr", "xm")[xr], yr)
        products = lax.dot_general(
            imgbuf[pl.ds(xr * cols, cols), :],
            capbuf[pl.ds(k * rows, rows), :],
            (((1,), (1,)), ((), ())),
            preferred_element_type=F32,
        )
        scale = consts[0:1, :]
        half_tanh = scale * jnp.tanh(products * scale + consts[1:2, :])
        if xr == 0:
            image = lax.broadcasted_iota(jnp.int32, (cols, rows), 0)
            half_tanh = half_tanh + jnp.where(image == midx[k : k + 1, :], -scale, scale)
        else:
            half_tanh = half_tanh + scale
        wt[pl.ds(xr * cols, cols), pl.ds(k * rows, rows)] = half_tanh.astype(BF16)

    def caption_part(k):
        part = lax.dot_general(
            wt[:, pl.ds(k * rows, rows)], imgbuf[...], (((0,), (0,)), ((), ())), preferred_element_type=F32
        )
        pown[k] = part[: 4 * R, :]
        d2ds[k] = part[4 * R :, :].astype(BF16)
        copies.send(("d", k), d2ds.at[k], d2dr.at[k], sibling)

    def z_first(k):
        copies.wait("d", k)
        step = sign(k)
        direct, late = (1, 3) if step == 1 else (3, 1)

        def total(zr):
            here = slice(zr * R, zr * R + R)
            return pown[k, here, :] + d2dr[k, here, :].astype(F32)

        zsrel[k] = total(2).astype(BF16)
        copies.send(("zrel", k), zsrel.at[k], zrrel.at[k], dev(0, 0, step))
        zsdir[k] = total(direct).astype(BF16)
        copies.send(("zdir", k), zsdir.at[k], zrdir.at[k], dev(0, 0, -step))
        pown[k, 0:R, :] = total(0)
        pown[k, late * R : late * R + R, :] = total(late)

    def z_late(k):
        copies.wait("zrel", k)
        step = sign(k)
        late = 3 if step == 1 else 1
        zsdep[k] = (pown[k, late * R : late * R + R, :] + zrrel[k].astype(F32)).astype(BF16)
        copies.send(("zdep", k), zsdep.at[k], zrdep.at[k], dev(0, 0, step))

    def project(first, sums, live):
        unit, inverse = normalize(cap_ref[pl.ds(first, R), :])
        grads = (sums - unit * jnp.sum(unit * sums, axis=1, keepdims=True)) * inverse
        cout[pl.ds(first, R), :] = jnp.where(live, grads, 0.0)

    def z_last(k):
        copies.wait("zdir", k)
        copies.wait("zdep", k)
        sums = pown[k, 0:R, :] + zrdir[k].astype(F32) + zrdep[k].astype(F32)
        gsb[pl.ds(k * R, R), :] = sums.astype(BF16)
        if k >= 2:
            t = k - 2
            count = kept - k * R
            row = lax.broadcasted_iota(jnp.int32, (R, count), 0).astype(F32)
            lane = (lax.broadcasted_iota(jnp.int32, (R, count), 1) + 2 * R).astype(F32)
            pick = jnp.where(row + tots[0:1, :count] == lane, 1.0, 0.0).astype(BF16)
            ts2[t] = jnp.dot(pick, gsb[pl.ds(k * R, count), :], preferred_element_type=F32).astype(BF16)
            copies.send(("tb", t), ts2.at[t], tr2.at[t], partner)
        live = before_total(k * R)
        project(k * R, jnp.where(live, sums, 0.0), live)

    def tail_last(t):
        copies.wait("tb", t)
        live = before_total(kept + t * R)
        project(kept + t * R, jnp.where(live, tr2[t].astype(F32), 0.0), live)

    def image_part(xr, h):
        first = xr * cols + h * two
        part = jnp.dot(wt[pl.ds(first, two), :], capbuf[...], preferred_element_type=F32)
        here = pl.ds(h * two, two)
        pairs = [(yr, pl.ds(place[yr] * n_img, n_img)) for yr in ((2, 0) if h == 0 else (1, 3))]
        if xr == 0:
            xown[here, :] = part
        elif xr == 2:
            xsrel[here, :] = part.astype(BF16)
            for yr, at in pairs:
                copies.send(("xrel", yr), xsrel.at[at], xrrel.at[at], dev(sign(yr)))
        elif (h == 0) == (xr == 3):
            xdep[here, :] = part
        else:
            xsdir[here, :] = part.astype(BF16)
            for yr, at in pairs:
                copies.send(("xdir", yr), xsdir.at[at], xrdir.at[at], dev(-sign(yr)))

    def x_late(yr):
        copies.wait("xrel", yr)
        here = pl.ds(place[yr] * n_img, n_img)
        xsdep[here, :] = (xdep[here, :] + xrrel[here, :].astype(F32)).astype(BF16)
        copies.send(("xdep", yr), xsdep.at[here], xrdep.at[here], dev(sign(yr)))

    low, high = pl.ds(0, half), pl.ds(half, half)

    def x_last(yr):
        copies.wait("xdir", yr)
        copies.wait("xdep", yr)
        here = pl.ds(place[yr] * n_img, n_img)
        sums = xown[here, :] + xrdir[here, :].astype(F32) + xrdep[here, :].astype(F32)
        if yr == 0:
            yown[...] = sums
        elif yr == 2:
            ysrel[...] = sums.astype(BF16)
            copies.send(("yrel", 0), ysrel.at[low], yrrel.at[low], partner)
            copies.send(("yrel", 1), ysrel.at[high], yrrel.at[high], dev(0, -near))
        elif yr == 1:
            ysdir[low, :] = sums[:half, :].astype(BF16)
            copies.send(("ydir", 1), ysdir.at[low], yrdir.at[low], partner)
            ydep[high, :] = sums[half:, :]
        else:
            ysdir[high, :] = sums[half:, :].astype(BF16)
            copies.send(("ydir", 3), ysdir.at[high], yrdir.at[high], dev(0, -near))
            ydep[low, :] = sums[:half, :]

    def y_late(part):
        copies.wait("yrel", part)
        here = (low, high)[part]
        ysdep[here, :] = (ydep[here, :] + yrrel[here, :].astype(F32)).astype(BF16)
        copies.send(("ydep", part), ysdep.at[here], yrdep.at[here], partner if part else dev(0, -near))

    def finish():
        for name in (("ydir", 1), ("ydir", 3), ("ydep", 0), ("ydep", 1)):
            copies.wait(*name)
        sums = yown[...] + yrdir[...].astype(F32) + yrdep[...].astype(F32)
        unit, inverse = normalize(img_ref[...])
        iout[...] = (sums - unit * jnp.sum(unit * sums, axis=1, keepdims=True)) * inverse

    actions = dict(
        sx=send_x, rx=relay_x, ry=relay_y, t=tail, p=pack, f=forward, A=weights, B=caption_part, C=image_part,
        zf=z_first, zl=z_late, zz=z_last, e=tail_last, xl=x_late, xz=x_last, yz=y_late, end=finish,
    )
    for kind, *numbers in ORDER:
        actions[kind](*numbers)
    copies.drain()


def shards(image_embed, caption_vectors, caption_counts, natural_log_multiplier, match_odds_offset):
    n_img, width = image_embed.shape
    n_slot = caption_vectors.shape[0]
    kept = 9 * n_img // 2
    nk, nt = kept // R, (n_slot - kept) // R
    cols, rows = 4 * n_img, 8 * R
    vmem = pl.BlockSpec(memory_space=pltpu.VMEM)
    smem = pl.BlockSpec(memory_space=pltpu.SMEM)

    def buf(*shape, dtype=BF16):
        return pltpu.VMEM((*shape, width), dtype)

    scratch = [
        buf(4 * cols),
        buf(nk * rows),
        buf(R),
        buf(nt, R),
        buf(nt * R),
        pltpu.VMEM((4 * cols, nk * rows), BF16),
        pltpu.VMEM((16, rows), jnp.int32),
        pltpu.VMEM((8, width), F32),
        pltpu.VMEM((8, rows), F32),
        buf(nk, 4 * R, dtype=F32),
        buf(nk, 4 * R),
        buf(nk, 4 * R),
        *[buf(nk, R)] * 6,
        buf(R, dtype=F32),
        buf(kept),
        buf(nt, R),
        buf(nt, R),
        *[buf(cols, dtype=F32)] * 2,
        *[buf(cols)] * 6,
        *[buf(n_img, dtype=F32)] * 2,
        *[buf(n_img)] * 6,
        pltpu.SemaphoreType.DMA((160,)),
        pltpu.SemaphoreType.DMA((160,)),
    ]
    return pl.pallas_call(
        kernel,
        out_shape=(
            jax.ShapeDtypeStruct((n_img, width), F32),
            jax.ShapeDtypeStruct((n_slot, width), F32),
        ),
        in_specs=[vmem, vmem, vmem, smem, smem],
        out_specs=(vmem, vmem),
        scratch_shapes=scratch,
        compiler_params=pltpu.CompilerParams(
            collective_id=0, has_side_effects=True, vmem_limit_bytes=60 * 1024 * 1024
        ),
    )(image_embed, caption_vectors, caption_counts.reshape(-1, 2 * n_img), natural_log_multiplier, match_odds_offset)


def solution(mesh):
    placed = (P(("blk", "group"), None), P(("blk", "group"), None), P(), P(), P())
    return jax.shard_map(
        shards,
        mesh=mesh,
        in_specs=placed,
        out_specs=(P(("blk", "group"), None), P(("blk", "group"), None)),
        check_vma=False,
    )
```

```python
import jax
import jax.numpy as jnp
from jax import lax
from jax.experimental import pallas as pl
from jax.experimental.pallas import tpu as pltpu
from jax.sharding import PartitionSpec as P

EPSILON = 1e-06
R = 32
F32 = jnp.float32
BF16 = jnp.bfloat16


YPOS = 2
ORDER = (
    ("sx", 0), ("t", 0), ("t", 1), ("p", 0), ("p", 1), ("t", 2), ("t", 3), ("t", 4), ("t", 5), ("t", 6), ("p", 2),
    ("f", 0, 1), ("f", 0, 3), ("rx", 0), ("p", 3), ("ry", 3), ("sx", 3), ("f", 1, 3), ("f", 1, 1), ("f", 2, 1),
    ("f", 2, 3), ("ry", 1), ("sx", 1), ("f", 3, 3), ("f", 0, 2), ("p", 4), ("f", 1, 2), ("f", 3, 1), ("rx", 3),
    ("p", 5), ("f", 2, 2), ("f", 3, 2), ("p", 6), ("f", 4, 1), ("rx", 1), ("f", 4, 3), ("p", 7), ("f", 5, 1),
    ("f", 5, 3), ("p", 8), ("f", 6, 1), ("f", 6, 3), ("sx", 2), ("A", 0, 0), ("A", 1, 0), ("A", 2, 0), ("A", 3, 0),
    ("f", 4, 2), ("f", 7, 3), ("A", 4, 0), ("f", 7, 1), ("f", 5, 2), ("f", 8, 1), ("A", 5, 0), ("f", 8, 3), ("rx", 2),
    ("A", 5, 1), ("A", 1, 1), ("A", 2, 3), ("A", 2, 1), ("A", 4, 3), ("A", 0, 3), ("A", 3, 1), ("A", 3, 3),
    ("A", 1, 3), ("A", 5, 3), ("f", 6, 2), ("A", 0, 1), ("A", 4, 1), ("f", 7, 2), ("f", 8, 2), ("A", 6, 0),
    ("A", 6, 1), ("A", 6, 3), ("A", 7, 3), ("A", 8, 3), ("A", 7, 1), ("A", 8, 1), ("A", 7, 0), ("A", 8, 0),
    ("C", 1, 0), ("A", 8, 2), ("B", 8), ("A", 6, 2), ("A", 4, 2), ("A", 1, 2), ("A", 2, 2), ("A", 0, 2), ("A", 7, 2),
    ("B", 7), ("A", 3, 2), ("A", 5, 2), ("zf", 8), ("B", 6), ("C", 2, 0), ("zf", 7), ("B", 5), ("C", 0, 1), ("zf", 6),
    ("C", 2, 1), ("zl", 8), ("C", 0, 0), ("zf", 5), ("B", 4), ("zl", 7), ("B", 3), ("C", 3, 0), ("xl", 2), ("zl", 6),
    ("C", 3, 1), ("zf", 4), ("zz", 8), ("zf", 3), ("zl", 5), ("B", 2), ("B", 1), ("zz", 7), ("xl", 0), ("C", 1, 1),
    ("xl", 1), ("zz", 6), ("zf", 2), ("B", 0), ("e", 6), ("xl", 3), ("xz", 2), ("zl", 4), ("zl", 3), ("zf", 1),
    ("e", 5), ("zf", 0), ("zz", 5), ("e", 4), ("zl", 2), ("xz", 1), ("yz", 1), ("zz", 4), ("zz", 3), ("e", 3),
    ("xz", 3), ("zl", 1), ("yz", 0), ("zl", 0), ("xz", 0), ("zz", 2), ("e", 2), ("zz", 1), ("zz", 0), ("end",),
    ("e", 1), ("e", 0),
)


def normalize(rows):
    values = rows.astype(F32)
    inverse = lax.rsqrt(jnp.sum(values * values, axis=1, keepdims=True) + EPSILON)
    return values * inverse, inverse


class Copies:
    def __init__(self, send_sem, recv_sem):
        self.send_sem, self.recv_sem, self.named, self.open = send_sem, recv_sem, {}, set()

    def send(self, name, src, dst, device):
        index = len(self.named)
        copy = pltpu.make_async_remote_copy(
            src_ref=src,
            dst_ref=dst,
            send_sem=self.send_sem.at[index],
            recv_sem=self.recv_sem.at[index],
            device_id=device,
            device_id_type=pl.DeviceIdType.MESH,
        )
        copy.start()
        self.named[name] = copy
        self.open.add(name)

    def wait(self, *name):
        if name in self.open:
            self.named[name].wait_recv()
            self.open.remove(name)

    def drain(self):
        for name, copy in self.named.items():
            self.wait(*name)
            copy.wait_send()


def kernel(
    img_hbm, cap_hbm, cnt_hbm, nlm_ref, bias_ref, iout, cout,
    img_ref, cap_ref, cnt_ref, load_sem, imgbuf, capbuf, head, tsend, trecv, wt, midx, tots, consts,
    pown, d2ds, d2dr, zsrel, zsdir, zsdep, zrrel, zrdir, zrdep, gs, gsb, ts2, tr2,
    xown, xdep, xsrel, xsdir, xsdep, xrrel, xrdir, xrdep,
    yown, ydep, ysrel, ysdir, ysdep, yrrel, yrdir, yrdep,
    send_sem, recv_sem,
):
    loads = [
        pltpu.make_async_copy(src, dst, load_sem.at[i])
        for i, (src, dst) in enumerate(((img_hbm, img_ref), (cap_hbm, cap_ref), (cnt_hbm, cnt_ref)))
    ]
    for load in loads:
        load.start()
    n_img, width = img_ref.shape
    n_slot = cap_ref.shape[0]
    kept = 9 * n_img // 2
    nk = kept // R
    nt = (n_slot - kept) // R
    cols = 4 * n_img
    rows = 8 * R
    half = n_img // 2
    blk = lax.axis_index("blk")
    grp = lax.axis_index("group")
    core, x, ylo = lax.rem(blk, 2), lax.rem(lax.div(blk, 2), 4), lax.div(blk, 8)
    z, yhi = lax.div(grp, 2), lax.rem(grp, 2)
    y = yhi * 2 + ylo
    near = 1 - 2 * ylo

    def dev(dx=0, dy=0, dz=0):
        px, py, pz = lax.rem(x + dx + 4, 4), lax.rem(y + dy + 4, 4), lax.rem(z + dz + 4, 4)
        return ((lax.rem(py, 2) * 4 + px) * 2 + core, pz * 2 + lax.div(py, 2))

    sibling = (blk + 1 - 2 * core, grp)
    partner = (((1 - ylo) * 4 + x) * 2 + core, grp)
    copies = Copies(send_sem, recv_sem)

    barrier = pltpu.get_barrier_semaphore()
    for device in (dev(1), dev(-1), dev(0, 1), dev(0, -1), dev(0, 0, 1), dev(0, 0, -1), sibling):
        pl.semaphore_signal(barrier, inc=1, device_id=device, device_id_type=pl.DeviceIdType.MESH)

    place = (0, 2, 1, 3)

    def img_at(xr, yr, first=0, count=n_img):
        return imgbuf.at[pl.ds(xr * cols + place[yr] * n_img + first, count)]

    def cap_at(k, core_rel, zr):
        return capbuf.at[pl.ds(k * rows + core_rel * 4 * R + zr * R, R)]

    def sign(index):
        return 1 if index % 2 == 0 else -1

    loads[0].wait()
    imgbuf[pl.ds(0, n_img), :] = normalize(img_ref[...])[0].astype(BF16)
    loads[1].wait()
    for t in range(nt):
        tsend[t] = normalize(cap_ref[pl.ds(kept + t * R, R), :])[0].astype(BF16)

    loads[2].wait()
    two = 2 * n_img
    image_row = lax.broadcasted_iota(jnp.int32, (n_img, two), 0)
    image_lane = lax.broadcasted_iota(jnp.int32, (n_img, two), 1)

    def running_ends(device, lanes):
        number = device[0] * 8 + device[1]
        counts = cnt_ref[pl.ds(lax.div(number, 2), 1), :].astype(F32)
        local = image_lane - lax.rem(number, 2) * n_img
        lower = jnp.where(jnp.logical_and(local >= 0, local <= image_row), counts, 0.0)
        return jnp.dot(lower.astype(BF16), jnp.ones((two, lanes), BF16), preferred_element_type=F32)

    own_ends = running_ends((blk, grp), width)
    tots[0:1, :] = own_ends[n_img - 1 :, :]
    log_row = jnp.full((1, rows), nlm_ref[0], F32)
    consts[0:1, :] = jnp.exp(log_row) * 0.5
    consts[1:2, :] = jnp.full((1, rows), bias_ref[0] * 0.5, F32)

    own_part = own_ends[:, :rows]
    pair_ends = running_ends(partner, rows)
    total_row = own_part[n_img - 1 :, :]
    lane = lax.broadcasted_iota(jnp.int32, (1, rows), 1)
    for k in range(nk):
        position = (lane + k * R).astype(F32)
        own_index = jnp.sum(jnp.where(own_part <= position, 1.0, 0.0), axis=0, keepdims=True)
        slot = position - total_row + float(kept)
        pair_index = jnp.sum(jnp.where(pair_ends <= slot, 1.0, 0.0), axis=0, keepdims=True)
        column = jnp.where(position < total_row, own_index, float(place[1] * n_img) + pair_index)
        midx[k : k + 1, :] = jnp.where(lane < R, column, -1.0).astype(jnp.int32)

    pl.semaphore_wait(barrier, 7)

    def before_total(first):
        position = lax.broadcasted_iota(jnp.int32, (R, width), 0) + first
        return position.astype(F32) < tots[0:1, :]

    def send_x(yr):
        if yr == 2:
            copies.wait("y2", 1)
            copies.wait("y2", 3)
        elif yr:
            copies.wait("y", yr)
        copies.send(("xp", yr), img_at(0, yr), img_at(1, yr), dev(1))
        copies.send(("xm", yr), img_at(0, yr), img_at(3, yr), dev(-1))

    def relay_x(yr):
        kind, xr = ("xp", 1) if yr % 2 == 0 else ("xm", 3)
        copies.wait(kind, yr)
        copies.send(("xr", yr), img_at(xr, yr), img_at(2, yr), dev(sign(yr)))

    def relay_y(yr):
        copies.wait("y", yr)
        first, step = (0, -near) if yr == 1 else (half, near)
        copies.send(("y2", yr), img_at(0, yr, first, half), img_at(0, 2, first, half), dev(0, step))

    def tail(t):
        copies.send(("t", t), tsend.at[t], trecv.at[pl.ds(t * R, R)], partner)
        if t == YPOS - 1:
            copies.send(("y", 1), img_at(0, 0), img_at(0, 1), partner)
            copies.send(("y", 3), img_at(0, 0), img_at(0, 3), dev(0, -near))

    def pack(k):
        block = normalize(cap_ref[pl.ds(k * R, R), :])[0]
        if k >= 2:
            copies.wait("t", k - 2)
            count = (k - 1) * R
            row = (lax.broadcasted_iota(jnp.int32, (R, count), 0) + k * R).astype(F32)
            lane = lax.broadcasted_iota(jnp.int32, (R, count), 1).astype(F32)
            pick = jnp.where(row - tots[0:1, :count] == lane, 1.0, 0.0).astype(BF16)
            moved = jnp.dot(pick, trecv[pl.ds(0, count), :], preferred_element_type=F32)
            block = jnp.where(before_total(k * R), block, moved)
        capbuf[pl.ds(k * rows, R), :] = block.astype(BF16)
        copies.send(("zp", k), cap_at(k, 0, 0), cap_at(k, 0, 1), dev(0, 0, 1))
        copies.send(("zm", k), cap_at(k, 0, 0), cap_at(k, 0, 3), dev(0, 0, -1))
        copies.send(("s", 0, k), cap_at(k, 0, 0), cap_at(k, 1, 0), sibling)

    def forward(k, zr):
        copies.wait(("", "zp", "zr", "zm")[zr], k)
        if zr != 2 and (zr == 1) == (k % 2 == 0):
            copies.send(("zr", k), cap_at(k, 0, zr), cap_at(k, 0, 2), dev(0, 0, sign(k)))
        copies.send(("s", zr, k), cap_at(k, 0, zr), cap_at(k, 1, zr), sibling)

    def weights(k, xr):
        for zr in range(4):
            copies.wait("s", zr, k)
        if xr == 0:
            for name in (("y", 1), ("y", 3), ("y2", 1), ("y2", 3)):
                copies.wait(*name)
        else:
            for yr in range(4):
                copies.wait(("", "xp", "xr", "xm")[xr], yr)
        products = lax.dot_general(
            imgbuf[pl.ds(xr * cols, cols), :],
            capbuf[pl.ds(k * rows, rows), :],
            (((1,), (1,)), ((), ())),
            preferred_element_type=F32,
        )
        scale = consts[0:1, :]
        half_tanh = scale * jnp.tanh(products * scale + consts[1:2, :])
        if xr == 0:
            image = lax.broadcasted_iota(jnp.int32, (cols, rows), 0)
            half_tanh = half_tanh + jnp.where(image == midx[k : k + 1, :], -scale, scale)
        else:
            half_tanh = half_tanh + scale
        wt[pl.ds(xr * cols, cols), pl.ds(k * rows, rows)] = half_tanh.astype(BF16)

    def caption_part(k):
        part = lax.dot_general(
            wt[:, pl.ds(k * rows, rows)], imgbuf[...], (((0,), (0,)), ((), ())), preferred_element_type=F32
        )
        pown[k] = part[: 4 * R, :]
        d2ds[k] = part[4 * R :, :].astype(BF16)
        copies.send(("d", k), d2ds.at[k], d2dr.at[k], sibling)

    def z_first(k):
        copies.wait("d", k)
        step = sign(k)
        direct, late = (1, 3) if step == 1 else (3, 1)

        def total(zr):
            here = slice(zr * R, zr * R + R)
            return pown[k, here, :] + d2dr[k, here, :].astype(F32)

        zsrel[k] = total(2).astype(BF16)
        copies.send(("zrel", k), zsrel.at[k], zrrel.at[k], dev(0, 0, step))
        zsdir[k] = total(direct).astype(BF16)
        copies.send(("zdir", k), zsdir.at[k], zrdir.at[k], dev(0, 0, -step))
        pown[k, 0:R, :] = total(0)
        pown[k, late * R : late * R + R, :] = total(late)

    def z_late(k):
        copies.wait("zrel", k)
        step = sign(k)
        late = 3 if step == 1 else 1
        zsdep[k] = (pown[k, late * R : late * R + R, :] + zrrel[k].astype(F32)).astype(BF16)
        copies.send(("zdep", k), zsdep.at[k], zrdep.at[k], dev(0, 0, step))

    def project(first, sums, live):
        unit, inverse = normalize(cap_ref[pl.ds(first, R), :])
        grads = (sums - unit * jnp.sum(unit * sums, axis=1, keepdims=True)) * inverse
        cout[pl.ds(first, R), :] = jnp.where(live, grads, 0.0)

    def z_last(k):
        copies.wait("zdir", k)
        copies.wait("zdep", k)
        sums = pown[k, 0:R, :] + zrdir[k].astype(F32) + zrdep[k].astype(F32)
        gsb[pl.ds(k * R, R), :] = sums.astype(BF16)
        if k >= 2:
            t = k - 2
            count = kept - k * R
            row = lax.broadcasted_iota(jnp.int32, (R, count), 0).astype(F32)
            lane = (lax.broadcasted_iota(jnp.int32, (R, count), 1) + 2 * R).astype(F32)
            pick = jnp.where(row + tots[0:1, :count] == lane, 1.0, 0.0).astype(BF16)
            ts2[t] = jnp.dot(pick, gsb[pl.ds(k * R, count), :], preferred_element_type=F32).astype(BF16)
            copies.send(("tb", t), ts2.at[t], tr2.at[t], partner)
        live = before_total(k * R)
        project(k * R, jnp.where(live, sums, 0.0), live)

    def tail_last(t):
        copies.wait("tb", t)
        live = before_total(kept + t * R)
        project(kept + t * R, jnp.where(live, tr2[t].astype(F32), 0.0), live)

    def image_part(xr, h):
        first = xr * cols + h * two
        part = jnp.dot(wt[pl.ds(first, two), :], capbuf[...], preferred_element_type=F32)
        here = pl.ds(h * two, two)
        pairs = [(yr, pl.ds(place[yr] * n_img, n_img)) for yr in ((2, 0) if h == 0 else (1, 3))]
        if xr == 0:
            xown[here, :] = part
        elif xr == 2:
            xsrel[here, :] = part.astype(BF16)
            for yr, at in pairs:
                copies.send(("xrel", yr), xsrel.at[at], xrrel.at[at], dev(sign(yr)))
        elif (h == 0) == (xr == 3):
            xdep[here, :] = part
        else:
            xsdir[here, :] = part.astype(BF16)
            for yr, at in pairs:
                copies.send(("xdir", yr), xsdir.at[at], xrdir.at[at], dev(-sign(yr)))

    def x_late(yr):
        copies.wait("xrel", yr)
        here = pl.ds(place[yr] * n_img, n_img)
        xsdep[here, :] = (xdep[here, :] + xrrel[here, :].astype(F32)).astype(BF16)
        copies.send(("xdep", yr), xsdep.at[here], xrdep.at[here], dev(sign(yr)))

    low, high = pl.ds(0, half), pl.ds(half, half)

    def x_last(yr):
        copies.wait("xdir", yr)
        copies.wait("xdep", yr)
        here = pl.ds(place[yr] * n_img, n_img)
        sums = xown[here, :] + xrdir[here, :].astype(F32) + xrdep[here, :].astype(F32)
        if yr == 0:
            yown[...] = sums
        elif yr == 2:
            ysrel[...] = sums.astype(BF16)
            copies.send(("yrel", 0), ysrel.at[low], yrrel.at[low], partner)
            copies.send(("yrel", 1), ysrel.at[high], yrrel.at[high], dev(0, -near))
        elif yr == 1:
            ysdir[low, :] = sums[:half, :].astype(BF16)
            copies.send(("ydir", 1), ysdir.at[low], yrdir.at[low], partner)
            ydep[high, :] = sums[half:, :]
        else:
            ysdir[high, :] = sums[half:, :].astype(BF16)
            copies.send(("ydir", 3), ysdir.at[high], yrdir.at[high], dev(0, -near))
            ydep[low, :] = sums[:half, :]

    def y_late(part):
        copies.wait("yrel", part)
        here = (low, high)[part]
        ysdep[here, :] = (ydep[here, :] + yrrel[here, :].astype(F32)).astype(BF16)
        copies.send(("ydep", part), ysdep.at[here], yrdep.at[here], partner if part else dev(0, -near))

    def finish():
        for name in (("ydir", 1), ("ydir", 3), ("ydep", 0), ("ydep", 1)):
            copies.wait(*name)
        sums = yown[...] + yrdir[...].astype(F32) + yrdep[...].astype(F32)
        unit, inverse = normalize(img_ref[...])
        iout[...] = (sums - unit * jnp.sum(unit * sums, axis=1, keepdims=True)) * inverse

    actions = dict(
        sx=send_x, rx=relay_x, ry=relay_y, t=tail, p=pack, f=forward, A=weights, B=caption_part, C=image_part,
        zf=z_first, zl=z_late, zz=z_last, e=tail_last, xl=x_late, xz=x_last, yz=y_late, end=finish,
    )
    for kind, *numbers in ORDER:
        actions[kind](*numbers)
    copies.drain()


def shards(image_embed, caption_vectors, caption_counts, natural_log_multiplier, match_odds_offset):
    n_img, width = image_embed.shape
    n_slot = caption_vectors.shape[0]
    kept = 9 * n_img // 2
    nk, nt = kept // R, (n_slot - kept) // R
    cols, rows = 4 * n_img, 8 * R
    vmem = pl.BlockSpec(memory_space=pltpu.VMEM)
    smem = pl.BlockSpec(memory_space=pltpu.SMEM)
    anywhere = pl.BlockSpec(memory_space=pl.ANY)

    def buf(*shape, dtype=BF16):
        return pltpu.VMEM((*shape, width), dtype)

    scratch = [
        buf(n_img),
        buf(n_slot),
        pltpu.VMEM((caption_counts.shape[0] // (2 * n_img), 2 * n_img), jnp.int32),
        pltpu.SemaphoreType.DMA((3,)),
        buf(4 * cols),
        buf(nk * rows),
        buf(R),
        buf(nt, R),
        buf(nt * R),
        pltpu.VMEM((4 * cols, nk * rows), BF16),
        pltpu.VMEM((16, rows), jnp.int32),
        pltpu.VMEM((8, width), F32),
        pltpu.VMEM((8, rows), F32),
        buf(nk, 4 * R, dtype=F32),
        buf(nk, 4 * R),
        buf(nk, 4 * R),
        *[buf(nk, R)] * 6,
        buf(R, dtype=F32),
        buf(kept),
        buf(nt, R),
        buf(nt, R),
        *[buf(cols, dtype=F32)] * 2,
        *[buf(cols)] * 6,
        *[buf(n_img, dtype=F32)] * 2,
        *[buf(n_img)] * 6,
        pltpu.SemaphoreType.DMA((160,)),
        pltpu.SemaphoreType.DMA((160,)),
    ]
    return pl.pallas_call(
        kernel,
        out_shape=(
            pltpu.VMEM((n_img, width), F32),
            pltpu.VMEM((n_slot, width), F32),
        ),
        in_specs=[anywhere, anywhere, anywhere, smem, smem],
        out_specs=(vmem, vmem),
        scratch_shapes=scratch,
        compiler_params=pltpu.CompilerParams(
            collective_id=0, has_side_effects=True, vmem_limit_bytes=60 * 1024 * 1024
        ),
    )(image_embed, caption_vectors, caption_counts.reshape(-1, 2 * n_img), natural_log_multiplier, match_odds_offset)


def solution(mesh):
    placed = (P(("blk", "group"), None), P(("blk", "group"), None), P(), P(), P())
    return jax.shard_map(
        shards,
        mesh=mesh,
        in_specs=placed,
        out_specs=(P(("blk", "group"), None), P(("blk", "group"), None)),
        check_vma=False,
    )
```

```python
import jax
import jax.numpy as jnp
from jax import lax
from jax.experimental import pallas as pl
from jax.experimental.pallas import tpu as pltpu
from jax.sharding import PartitionSpec as P

EPSILON = 1e-06
R = 32
F32 = jnp.float32
BF16 = jnp.bfloat16


SETUP = ("p", 2)
YPOS = 4
ORDER = (
    ("sx", 0), ("t", 0), ("t", 1), ("p", 0), ("p", 1), ("t", 2), ("t", 3), ("t", 4), ("p", 2), ("f", 0, 1),
    ("f", 0, 3), ("rx", 0), ("p", 3), ("f", 1, 3), ("f", 1, 1), ("sx", 3), ("ry", 3), ("t", 5), ("t", 6), ("p", 4),
    ("f", 2, 1), ("f", 2, 3), ("p", 5), ("f", 0, 2), ("f", 3, 3), ("f", 1, 2), ("f", 3, 1), ("rx", 3), ("ry", 1),
    ("sx", 1), ("f", 4, 1), ("f", 4, 3), ("p", 6), ("f", 2, 2), ("f", 5, 3), ("sx", 2), ("A", 0, 0), ("f", 3, 2),
    ("A", 2, 0), ("f", 5, 1), ("A", 1, 0), ("p", 7), ("A", 3, 0), ("f", 4, 2), ("f", 6, 3), ("p", 8), ("A", 4, 0),
    ("f", 5, 2), ("f", 6, 1), ("rx", 1), ("A", 5, 0), ("f", 7, 1), ("f", 7, 3), ("rx", 2), ("A", 1, 1), ("A", 4, 1),
    ("A", 3, 1), ("A", 0, 1), ("A", 5, 1), ("A", 2, 1), ("f", 8, 1), ("f", 8, 3), ("A", 2, 3), ("A", 3, 3),
    ("A", 1, 3), ("A", 0, 3), ("f", 6, 2), ("A", 4, 3), ("A", 5, 3), ("f", 7, 2), ("A", 6, 0), ("A", 6, 1),
    ("A", 6, 3), ("A", 7, 1), ("A", 7, 3), ("f", 8, 2), ("A", 7, 0), ("A", 0, 2), ("A", 7, 2), ("B", 7), ("A", 8, 1),
    ("A", 2, 2), ("A", 8, 2), ("A", 8, 0), ("A", 8, 3), ("B", 8), ("C", 1, 0), ("A", 4, 2), ("A", 3, 2), ("zf", 7),
    ("A", 1, 2), ("A", 6, 2), ("B", 6), ("zf", 8), ("A", 5, 2), ("C", 2, 0), ("B", 5), ("C", 0, 1), ("zf", 6),
    ("zl", 7), ("B", 2), ("C", 2, 1), ("zl", 8), ("zf", 5), ("B", 1), ("B", 4), ("B", 3), ("zl", 6), ("C", 3, 0),
    ("xl", 2), ("C", 3, 1), ("zz", 8), ("zz", 7), ("zf", 4), ("C", 1, 1), ("xl", 0), ("xl", 1), ("zl", 5), ("zf", 3),
    ("B", 0), ("zf", 2), ("zz", 6), ("C", 0, 0), ("e", 6), ("zl", 4), ("xz", 2), ("xl", 3), ("zf", 0), ("e", 5),
    ("zz", 5), ("e", 4), ("zl", 3), ("zl", 2), ("zf", 1), ("xz", 1), ("yz", 1), ("zz", 4), ("e", 3), ("zl", 0),
    ("xz", 3), ("yz", 0), ("zz", 3), ("zz", 2), ("zl", 1), ("xz", 0), ("e", 2), ("zz", 0), ("end",), ("e", 1),
    ("zz", 1), ("e", 0),
)


def normalize(rows):
    values = rows.astype(F32)
    inverse = lax.rsqrt(jnp.sum(values * values, axis=1, keepdims=True) + EPSILON)
    return values * inverse, inverse


class Copies:
    def __init__(self, send_sem, recv_sem):
        self.send_sem, self.recv_sem, self.named, self.open = send_sem, recv_sem, {}, set()

    def send(self, name, src, dst, device):
        index = len(self.named)
        copy = pltpu.make_async_remote_copy(
            src_ref=src,
            dst_ref=dst,
            send_sem=self.send_sem.at[index],
            recv_sem=self.recv_sem.at[index],
            device_id=device,
            device_id_type=pl.DeviceIdType.MESH,
        )
        copy.start()
        self.named[name] = copy
        self.open.add(name)

    def wait(self, *name):
        if name in self.open:
            self.named[name].wait_recv()
            self.open.remove(name)

    def drain(self):
        for name, copy in self.named.items():
            self.wait(*name)
            copy.wait_send()


def kernel(
    img_hbm, cap_hbm, cnt_hbm, nlm_ref, bias_ref, iout, cout,
    img_ref, cap_ref, cnt_ref, load_sem, imgbuf, capbuf, head, tsend, trecv, wt, midx, tots, consts,
    pown, d2ds, d2dr, zsrel, zsdir, zsdep, zrrel, zrdir, zrdep, gs, gsb, ts2, tr2,
    xown, xdep, xsrel, xsdir, xsdep, xrrel, xrdir, xrdep,
    yown, ydep, ysrel, ysdir, ysdep, yrrel, yrdir, yrdep,
    send_sem, recv_sem,
):
    loads = [
        pltpu.make_async_copy(src, dst, load_sem.at[i])
        for i, (src, dst) in enumerate(((img_hbm, img_ref), (cap_hbm, cap_ref), (cnt_hbm, cnt_ref)))
    ]
    for load in loads:
        load.start()
    n_img, width = img_ref.shape
    n_slot = cap_ref.shape[0]
    kept = 9 * n_img // 2
    nk = kept // R
    nt = (n_slot - kept) // R
    cols = 4 * n_img
    rows = 8 * R
    half = n_img // 2
    two = 2 * n_img
    blk = lax.axis_index("blk")
    grp = lax.axis_index("group")
    core, x, ylo = lax.rem(blk, 2), lax.rem(lax.div(blk, 2), 4), lax.div(blk, 8)
    z, yhi = lax.div(grp, 2), lax.rem(grp, 2)
    y = yhi * 2 + ylo
    near = 1 - 2 * ylo

    def dev(dx=0, dy=0, dz=0):
        px, py, pz = lax.rem(x + dx + 4, 4), lax.rem(y + dy + 4, 4), lax.rem(z + dz + 4, 4)
        return ((lax.rem(py, 2) * 4 + px) * 2 + core, pz * 2 + lax.div(py, 2))

    sibling = (blk + 1 - 2 * core, grp)
    partner = (((1 - ylo) * 4 + x) * 2 + core, grp)
    copies = Copies(send_sem, recv_sem)

    barrier = pltpu.get_barrier_semaphore()
    for device in (dev(1), dev(-1), dev(0, 1), dev(0, -1), dev(0, 0, 1), dev(0, 0, -1), sibling):
        pl.semaphore_signal(barrier, inc=1, device_id=device, device_id_type=pl.DeviceIdType.MESH)

    place = (0, 2, 1, 3)

    def img_at(xr, yr, first=0, count=n_img):
        return imgbuf.at[pl.ds(xr * cols + place[yr] * n_img + first, count)]

    def cap_at(k, core_rel, zr):
        return capbuf.at[pl.ds(k * rows + core_rel * 4 * R + zr * R, R)]

    def sign(index):
        return 1 if index % 2 == 0 else -1

    loads[0].wait()
    imgbuf[pl.ds(0, n_img), :] = normalize(img_ref[...])[0].astype(BF16)
    loads[1].wait()
    def make_tail(t):
        tsend[t] = normalize(cap_ref[pl.ds(kept + t * R, R), :])[0].astype(BF16)

    def make_head(k):
        capbuf[pl.ds(k * rows, R), :] = normalize(cap_ref[pl.ds(k * R, R), :])[0].astype(BF16)

    for i in range(2):
        make_tail(i)
        make_head(i)
    pl.semaphore_wait(barrier, 7)

    def before_total(first):
        position = lax.broadcasted_iota(jnp.int32, (R, width), 0) + first
        return position.astype(F32) < tots[0:1, :]

    def setup():
        loads[2].wait()
        image_row = lax.broadcasted_iota(jnp.int32, (n_img, two), 0)
        image_lane = lax.broadcasted_iota(jnp.int32, (n_img, two), 1)

        def running_ends(device, lanes):
            number = device[0] * 8 + device[1]
            counts = cnt_ref[pl.ds(lax.div(number, 2), 1), :].astype(F32)
            local = image_lane - lax.rem(number, 2) * n_img
            lower = jnp.where(jnp.logical_and(local >= 0, local <= image_row), counts, 0.0)
            return jnp.dot(lower.astype(BF16), jnp.ones((two, lanes), BF16), preferred_element_type=F32)

        own_ends = running_ends((blk, grp), width)
        tots[0:1, :] = own_ends[n_img - 1 :, :]
        log_row = jnp.full((1, rows), nlm_ref[0], F32)
        consts[0:1, :] = jnp.exp(log_row) * 0.5
        consts[1:2, :] = jnp.full((1, rows), bias_ref[0] * 0.5, F32)

        own_part = own_ends[:, :rows]
        pair_ends = running_ends(partner, rows)
        total_row = own_part[n_img - 1 :, :]
        lane = lax.broadcasted_iota(jnp.int32, (1, rows), 1)
        for k in range(nk):
            position = (lane + k * R).astype(F32)
            own_index = jnp.sum(jnp.where(own_part <= position, 1.0, 0.0), axis=0, keepdims=True)
            slot = position - total_row + float(kept)
            pair_index = jnp.sum(jnp.where(pair_ends <= slot, 1.0, 0.0), axis=0, keepdims=True)
            column = jnp.where(position < total_row, own_index, float(place[1] * n_img) + pair_index)
            midx[k : k + 1, :] = jnp.where(lane < R, column, -1.0).astype(jnp.int32)

    def send_x(yr):
        if yr == 2:
            copies.wait("y2", 1)
            copies.wait("y2", 3)
        elif yr:
            copies.wait("y", yr)
        copies.send(("xp", yr), img_at(0, yr), img_at(1, yr), dev(1))
        copies.send(("xm", yr), img_at(0, yr), img_at(3, yr), dev(-1))

    def relay_x(yr):
        kind, xr = ("xp", 1) if yr % 2 == 0 else ("xm", 3)
        copies.wait(kind, yr)
        copies.send(("xr", yr), img_at(xr, yr), img_at(2, yr), dev(sign(yr)))

    def relay_y(yr):
        copies.wait("y", yr)
        first, step = (0, -near) if yr == 1 else (half, near)
        copies.send(("y2", yr), img_at(0, yr, first, half), img_at(0, 2, first, half), dev(0, step))

    def tail(t):
        if t >= 2:
            make_tail(t)
        copies.send(("t", t), tsend.at[t], trecv.at[pl.ds(t * R, R)], partner)
        if t == YPOS - 1:
            copies.send(("y", 1), img_at(0, 0), img_at(0, 1), partner)
            copies.send(("y", 3), img_at(0, 0), img_at(0, 3), dev(0, -near))

    def pack(k):
        if k >= 2:
            block = normalize(cap_ref[pl.ds(k * R, R), :])[0]
            copies.wait("t", k - 2)
            count = (k - 1) * R
            row = (lax.broadcasted_iota(jnp.int32, (R, count), 0) + k * R).astype(F32)
            lane = lax.broadcasted_iota(jnp.int32, (R, count), 1).astype(F32)
            pick = jnp.where(row - tots[0:1, :count] == lane, 1.0, 0.0).astype(BF16)
            moved = jnp.dot(pick, trecv[pl.ds(0, count), :], preferred_element_type=F32)
            block = jnp.where(before_total(k * R), block, moved)
            capbuf[pl.ds(k * rows, R), :] = block.astype(BF16)
        copies.send(("zp", k), cap_at(k, 0, 0), cap_at(k, 0, 1), dev(0, 0, 1))
        copies.send(("zm", k), cap_at(k, 0, 0), cap_at(k, 0, 3), dev(0, 0, -1))
        copies.send(("s", 0, k), cap_at(k, 0, 0), cap_at(k, 1, 0), sibling)

    def forward(k, zr):
        copies.wait(("", "zp", "zr", "zm")[zr], k)
        if zr != 2 and (zr == 1) == (k % 2 == 0):
            copies.send(("zr", k), cap_at(k, 0, zr), cap_at(k, 0, 2), dev(0, 0, sign(k)))
        copies.send(("s", zr, k), cap_at(k, 0, zr), cap_at(k, 1, zr), sibling)

    def weights(k, xr):
        for zr in range(4):
            copies.wait("s", zr, k)
        if xr == 0:
            for name in (("y", 1), ("y", 3), ("y2", 1), ("y2", 3)):
                copies.wait(*name)
        else:
            for yr in range(4):
                copies.wait(("", "xp", "xr", "xm")[xr], yr)
        products = lax.dot_general(
            imgbuf[pl.ds(xr * cols, cols), :],
            capbuf[pl.ds(k * rows, rows), :],
            (((1,), (1,)), ((), ())),
            preferred_element_type=F32,
        )
        scale = consts[0:1, :]
        half_tanh = scale * jnp.tanh(products * scale + consts[1:2, :])
        if xr == 0:
            image = lax.broadcasted_iota(jnp.int32, (cols, rows), 0)
            half_tanh = half_tanh + jnp.where(image == midx[k : k + 1, :], -scale, scale)
        else:
            half_tanh = half_tanh + scale
        wt[pl.ds(xr * cols, cols), pl.ds(k * rows, rows)] = half_tanh.astype(BF16)

    def caption_part(k):
        part = lax.dot_general(
            wt[:, pl.ds(k * rows, rows)], imgbuf[...], (((0,), (0,)), ((), ())), preferred_element_type=F32
        )
        pown[k] = part[: 4 * R, :]
        d2ds[k] = part[4 * R :, :].astype(BF16)
        copies.send(("d", k), d2ds.at[k], d2dr.at[k], sibling)

    def z_first(k):
        copies.wait("d", k)
        step = sign(k)
        direct, late = (1, 3) if step == 1 else (3, 1)

        def total(zr):
            here = slice(zr * R, zr * R + R)
            return pown[k, here, :] + d2dr[k, here, :].astype(F32)

        zsrel[k] = total(2).astype(BF16)
        copies.send(("zrel", k), zsrel.at[k], zrrel.at[k], dev(0, 0, step))
        zsdir[k] = total(direct).astype(BF16)
        copies.send(("zdir", k), zsdir.at[k], zrdir.at[k], dev(0, 0, -step))
        pown[k, 0:R, :] = total(0)
        pown[k, late * R : late * R + R, :] = total(late)

    def z_late(k):
        copies.wait("zrel", k)
        step = sign(k)
        late = 3 if step == 1 else 1
        zsdep[k] = (pown[k, late * R : late * R + R, :] + zrrel[k].astype(F32)).astype(BF16)
        copies.send(("zdep", k), zsdep.at[k], zrdep.at[k], dev(0, 0, step))

    def project(first, sums, live):
        unit, inverse = normalize(cap_ref[pl.ds(first, R), :])
        grads = (sums - unit * jnp.sum(unit * sums, axis=1, keepdims=True)) * inverse
        cout[pl.ds(first, R), :] = jnp.where(live, grads, 0.0)

    def z_last(k):
        copies.wait("zdir", k)
        copies.wait("zdep", k)
        sums = pown[k, 0:R, :] + zrdir[k].astype(F32) + zrdep[k].astype(F32)
        gsb[pl.ds(k * R, R), :] = sums.astype(BF16)
        if k >= 2:
            t = k - 2
            count = kept - k * R
            row = lax.broadcasted_iota(jnp.int32, (R, count), 0).astype(F32)
            lane = (lax.broadcasted_iota(jnp.int32, (R, count), 1) + 2 * R).astype(F32)
            pick = jnp.where(row + tots[0:1, :count] == lane, 1.0, 0.0).astype(BF16)
            ts2[t] = jnp.dot(pick, gsb[pl.ds(k * R, count), :], preferred_element_type=F32).astype(BF16)
            copies.send(("tb", t), ts2.at[t], tr2.at[t], partner)
        live = before_total(k * R)
        project(k * R, jnp.where(live, sums, 0.0), live)

    def tail_last(t):
        copies.wait("tb", t)
        live = before_total(kept + t * R)
        project(kept + t * R, jnp.where(live, tr2[t].astype(F32), 0.0), live)

    def image_part(xr, h):
        first = xr * cols + h * two
        part = jnp.dot(wt[pl.ds(first, two), :], capbuf[...], preferred_element_type=F32)
        here = pl.ds(h * two, two)
        pairs = [(yr, pl.ds(place[yr] * n_img, n_img)) for yr in ((2, 0) if h == 0 else (1, 3))]
        if xr == 0:
            xown[here, :] = part
        elif xr == 2:
            xsrel[here, :] = part.astype(BF16)
            for yr, at in pairs:
                copies.send(("xrel", yr), xsrel.at[at], xrrel.at[at], dev(sign(yr)))
        elif (h == 0) == (xr == 3):
            xdep[here, :] = part
        else:
            xsdir[here, :] = part.astype(BF16)
            for yr, at in pairs:
                copies.send(("xdir", yr), xsdir.at[at], xrdir.at[at], dev(-sign(yr)))

    def x_late(yr):
        copies.wait("xrel", yr)
        here = pl.ds(place[yr] * n_img, n_img)
        xsdep[here, :] = (xdep[here, :] + xrrel[here, :].astype(F32)).astype(BF16)
        copies.send(("xdep", yr), xsdep.at[here], xrdep.at[here], dev(sign(yr)))

    low, high = pl.ds(0, half), pl.ds(half, half)

    def x_last(yr):
        copies.wait("xdir", yr)
        copies.wait("xdep", yr)
        here = pl.ds(place[yr] * n_img, n_img)
        sums = xown[here, :] + xrdir[here, :].astype(F32) + xrdep[here, :].astype(F32)
        if yr == 0:
            yown[...] = sums
        elif yr == 2:
            ysrel[...] = sums.astype(BF16)
            copies.send(("yrel", 0), ysrel.at[low], yrrel.at[low], partner)
            copies.send(("yrel", 1), ysrel.at[high], yrrel.at[high], dev(0, -near))
        elif yr == 1:
            ysdir[low, :] = sums[:half, :].astype(BF16)
            copies.send(("ydir", 1), ysdir.at[low], yrdir.at[low], partner)
            ydep[high, :] = sums[half:, :]
        else:
            ysdir[high, :] = sums[half:, :].astype(BF16)
            copies.send(("ydir", 3), ysdir.at[high], yrdir.at[high], dev(0, -near))
            ydep[low, :] = sums[:half, :]

    def y_late(part):
        copies.wait("yrel", part)
        here = (low, high)[part]
        ysdep[here, :] = (ydep[here, :] + yrrel[here, :].astype(F32)).astype(BF16)
        copies.send(("ydep", part), ysdep.at[here], yrdep.at[here], partner if part else dev(0, -near))

    def finish():
        for name in (("ydir", 1), ("ydir", 3), ("ydep", 0), ("ydep", 1)):
            copies.wait(*name)
        sums = yown[...] + yrdir[...].astype(F32) + yrdep[...].astype(F32)
        unit, inverse = normalize(img_ref[...])
        iout[...] = (sums - unit * jnp.sum(unit * sums, axis=1, keepdims=True)) * inverse

    actions = dict(
        sx=send_x, rx=relay_x, ry=relay_y, t=tail, p=pack, f=forward, A=weights, B=caption_part, C=image_part,
        zf=z_first, zl=z_late, zz=z_last, e=tail_last, xl=x_late, xz=x_last, yz=y_late, end=finish,
    )
    for kind, *numbers in ORDER:
        if (kind, *numbers) == SETUP:
            setup()
        actions[kind](*numbers)
    copies.drain()


def shards(image_embed, caption_vectors, caption_counts, natural_log_multiplier, match_odds_offset):
    n_img, width = image_embed.shape
    n_slot = caption_vectors.shape[0]
    kept = 9 * n_img // 2
    nk, nt = kept // R, (n_slot - kept) // R
    cols, rows = 4 * n_img, 8 * R
    vmem = pl.BlockSpec(memory_space=pltpu.VMEM)
    smem = pl.BlockSpec(memory_space=pltpu.SMEM)
    anywhere = pl.BlockSpec(memory_space=pl.ANY)

    def buf(*shape, dtype=BF16):
        return pltpu.VMEM((*shape, width), dtype)

    scratch = [
        buf(n_img),
        buf(n_slot),
        pltpu.VMEM((caption_counts.shape[0] // (2 * n_img), 2 * n_img), jnp.int32),
        pltpu.SemaphoreType.DMA((3,)),
        buf(4 * cols),
        buf(nk * rows),
        buf(R),
        buf(nt, R),
        buf(nt * R),
        pltpu.VMEM((4 * cols, nk * rows), BF16),
        pltpu.VMEM((16, rows), jnp.int32),
        pltpu.VMEM((8, width), F32),
        pltpu.VMEM((8, rows), F32),
        buf(nk, 4 * R, dtype=F32),
        buf(nk, 4 * R),
        buf(nk, 4 * R),
        *[buf(nk, R)] * 6,
        buf(R, dtype=F32),
        buf(kept),
        buf(nt, R),
        buf(nt, R),
        *[buf(cols, dtype=F32)] * 2,
        *[buf(cols)] * 6,
        *[buf(n_img, dtype=F32)] * 2,
        *[buf(n_img)] * 6,
        pltpu.SemaphoreType.DMA((160,)),
        pltpu.SemaphoreType.DMA((160,)),
    ]
    return pl.pallas_call(
        kernel,
        out_shape=(
            pltpu.VMEM((n_img, width), F32),
            pltpu.VMEM((n_slot, width), F32),
        ),
        in_specs=[anywhere, anywhere, anywhere, smem, smem],
        out_specs=(vmem, vmem),
        scratch_shapes=scratch,
        compiler_params=pltpu.CompilerParams(
            collective_id=0, has_side_effects=True, vmem_limit_bytes=60 * 1024 * 1024
        ),
    )(image_embed, caption_vectors, caption_counts.reshape(-1, 2 * n_img), natural_log_multiplier, match_odds_offset)


def solution(mesh):
    placed = (P(("blk", "group"), None), P(("blk", "group"), None), P(), P(), P())
    return jax.shard_map(
        shards,
        mesh=mesh,
        in_specs=placed,
        out_specs=(P(("blk", "group"), None), P(("blk", "group"), None)),
        check_vma=False,
    )
```

```python
import jax
import jax.numpy as jnp
from jax import lax
from jax.experimental import pallas as pl
from jax.experimental.pallas import tpu as pltpu
from jax.sharding import PartitionSpec as P

EPSILON = 1e-06
R = 32
F32 = jnp.float32
BF16 = jnp.bfloat16


SETUP = ("p", 2)
YPOS = 4
ORDER = (
    ("sx", 0), ("t", 0), ("t", 1), ("p", 0), ("p", 1), ("t", 2), ("t", 3), ("t", 4), ("p", 2), ("f", 0, 3),
    ("f", 0, 1), ("rx", 0), ("p", 3), ("f", 1, 3), ("f", 1, 1), ("sx", 3), ("ry", 3), ("t", 5), ("t", 6), ("p", 4),
    ("f", 2, 1), ("f", 2, 3), ("p", 5), ("f", 0, 2), ("f", 3, 3), ("f", 1, 2), ("f", 3, 1), ("gy", 3, 0), ("rx", 3),
    ("ry", 1), ("sx", 1), ("f", 4, 3), ("f", 4, 1), ("p", 6), ("gy", 1, 0), ("f", 2, 2), ("f", 5, 3), ("A", 0, 0),
    ("A", 2, 0), ("f", 3, 2), ("f", 5, 1), ("A", 1, 0), ("p", 7), ("gy", 1, 1), ("A", 3, 0), ("f", 4, 2), ("f", 6, 3),
    ("p", 8), ("A", 4, 0), ("f", 5, 2), ("f", 6, 1), ("gy", 3, 1), ("rx", 1), ("A", 5, 0), ("f", 7, 1), ("f", 7, 3),
    ("rx", 2), ("A", 1, 1), ("A", 3, 1), ("A", 4, 1), ("A", 0, 1), ("A", 2, 1), ("A", 5, 1), ("f", 8, 1), ("f", 8, 3),
    ("f", 6, 2), ("A", 3, 3), ("A", 2, 3), ("A", 4, 3), ("A", 1, 3), ("f", 7, 2), ("A", 0, 3), ("A", 5, 3),
    ("A", 6, 0), ("A", 6, 1), ("A", 6, 3), ("A", 7, 3), ("A", 7, 1), ("A", 7, 0), ("f", 8, 2), ("A", 0, 2),
    ("A", 7, 2), ("B", 7), ("A", 8, 1), ("A", 8, 0), ("A", 8, 2), ("A", 2, 2), ("A", 8, 3), ("B", 8), ("C", 1, 0),
    ("zf", 7), ("A", 4, 2), ("A", 6, 2), ("B", 6), ("zf", 8), ("A", 3, 2), ("A", 1, 2), ("A", 5, 2), ("C", 2, 0),
    ("B", 5), ("zf", 6), ("C", 2, 1), ("zl", 7), ("B", 3), ("C", 3, 0), ("zl", 8), ("zf", 5), ("B", 4), ("C", 1, 1),
    ("zl", 6), ("zf", 3), ("xl", 2), ("B", 1), ("C", 3, 1), ("zf", 4), ("zz", 8), ("zz", 7), ("B", 2), ("zl", 5),
    ("zf", 1), ("B", 0), ("xl", 1), ("xl", 0), ("zl", 3), ("C", 0, 1), ("zz", 6), ("zf", 2), ("C", 0, 0), ("e", 6),
    ("xz", 2), ("xl", 3), ("zz", 5), ("e", 5), ("zl", 4), ("zf", 0), ("zl", 1), ("e", 4), ("xz", 1), ("yz", 1),
    ("zl", 2), ("e", 3), ("zz", 4), ("zz", 3), ("xz", 3), ("yz", 0), ("zl", 0), ("zz", 1), ("xz", 0), ("zz", 2),
    ("e", 2), ("zz", 0), ("e", 1), ("end",), ("e", 0),
)


def normalize(rows):
    values = rows.astype(F32)
    inverse = lax.rsqrt(jnp.sum(values * values, axis=1, keepdims=True) + EPSILON)
    return values * inverse, inverse


class Copies:
    def __init__(self, send_sem, recv_sem):
        self.send_sem, self.recv_sem, self.named, self.open = send_sem, recv_sem, {}, set()

    def send(self, name, src, dst, device):
        index = len(self.named)
        copy = pltpu.make_async_remote_copy(
            src_ref=src,
            dst_ref=dst,
            send_sem=self.send_sem.at[index],
            recv_sem=self.recv_sem.at[index],
            device_id=device,
            device_id_type=pl.DeviceIdType.MESH,
        )
        copy.start()
        self.named[name] = copy
        self.open.add(name)

    def wait(self, *name):
        if name in self.open:
            self.named[name].wait_recv()
            self.open.remove(name)

    def drain(self):
        for name, copy in self.named.items():
            self.wait(*name)
            copy.wait_send()


def kernel(
    img_hbm, cap_hbm, cnt_hbm, nlm_ref, bias_ref, iout, cout,
    img_ref, cap_ref, cnt_ref, load_sem, imgbuf, capbuf, head, tsend, trecv, wt, midx, tots, consts,
    pown, d2ds, d2dr, zsrel, zsdir, zsdep, zrrel, zrdir, zrdep, gs, gsb, ts2, tr2,
    xown, xdep, xsrel, xsdir, xsdep, xrrel, xrdir, xrdep,
    yown, ydep, ysrel, ysdir, ysdep, yrrel, yrdir, yrdep,
    send_sem, recv_sem,
):
    loads = [
        pltpu.make_async_copy(src, dst, load_sem.at[i])
        for i, (src, dst) in enumerate(((img_hbm, img_ref), (cap_hbm, cap_ref), (cnt_hbm, cnt_ref)))
    ]
    for load in loads:
        load.start()
    n_img, width = img_ref.shape
    n_slot = cap_ref.shape[0]
    kept = 9 * n_img // 2
    nk = kept // R
    nt = (n_slot - kept) // R
    cols = 4 * n_img
    rows = 8 * R
    half = n_img // 2
    two = 2 * n_img
    blk = lax.axis_index("blk")
    grp = lax.axis_index("group")
    core, x, ylo = lax.rem(blk, 2), lax.rem(lax.div(blk, 2), 4), lax.div(blk, 8)
    z, yhi = lax.div(grp, 2), lax.rem(grp, 2)
    y = yhi * 2 + ylo
    near = 1 - 2 * ylo

    def dev(dx=0, dy=0, dz=0):
        px, py, pz = lax.rem(x + dx + 4, 4), lax.rem(y + dy + 4, 4), lax.rem(z + dz + 4, 4)
        return ((lax.rem(py, 2) * 4 + px) * 2 + core, pz * 2 + lax.div(py, 2))

    sibling = (blk + 1 - 2 * core, grp)
    partner = (((1 - ylo) * 4 + x) * 2 + core, grp)
    copies = Copies(send_sem, recv_sem)

    barrier = pltpu.get_barrier_semaphore()
    for device in (dev(1), dev(-1), dev(0, 1), dev(0, -1), dev(0, 0, 1), dev(0, 0, -1), sibling):
        pl.semaphore_signal(barrier, inc=1, device_id=device, device_id_type=pl.DeviceIdType.MESH)

    place = (0, 2, 1, 3)

    def img_at(xr, yr, first=0, count=n_img):
        return imgbuf.at[pl.ds(xr * cols + place[yr] * n_img + first, count)]

    def cap_at(k, core_rel, zr):
        return capbuf.at[pl.ds(k * rows + core_rel * 4 * R + zr * R, R)]

    def sign(index):
        return 1 if index % 2 == 0 else -1

    loads[0].wait()
    imgbuf[pl.ds(0, n_img), :] = normalize(img_ref[...])[0].astype(BF16)
    loads[1].wait()
    def make_tail(t):
        tsend[t] = normalize(cap_ref[pl.ds(kept + t * R, R), :])[0].astype(BF16)

    def make_head(k):
        capbuf[pl.ds(k * rows, R), :] = normalize(cap_ref[pl.ds(k * R, R), :])[0].astype(BF16)

    for i in range(2):
        make_tail(i)
        make_head(i)
    pl.semaphore_wait(barrier, 7)

    def before_total(first):
        position = lax.broadcasted_iota(jnp.int32, (R, width), 0) + first
        return position.astype(F32) < tots[0:1, :]

    def setup():
        loads[2].wait()
        image_row = lax.broadcasted_iota(jnp.int32, (n_img, two), 0)
        image_lane = lax.broadcasted_iota(jnp.int32, (n_img, two), 1)

        def running_ends(device, lanes):
            number = device[0] * 8 + device[1]
            counts = cnt_ref[pl.ds(lax.div(number, 2), 1), :].astype(F32)
            local = image_lane - lax.rem(number, 2) * n_img
            lower = jnp.where(jnp.logical_and(local >= 0, local <= image_row), counts, 0.0)
            return jnp.dot(lower.astype(BF16), jnp.ones((two, lanes), BF16), preferred_element_type=F32)

        own_ends = running_ends((blk, grp), width)
        tots[0:1, :] = own_ends[n_img - 1 :, :]
        log_row = jnp.full((1, rows), nlm_ref[0], F32)
        consts[0:1, :] = jnp.exp(log_row) * 0.5
        consts[1:2, :] = jnp.full((1, rows), bias_ref[0] * 0.5, F32)

        own_part = own_ends[:, :rows]
        pair_ends = running_ends(partner, rows)
        total_row = own_part[n_img - 1 :, :]
        lane = lax.broadcasted_iota(jnp.int32, (1, rows), 1)
        for k in range(nk):
            position = (lane + k * R).astype(F32)
            own_index = jnp.sum(jnp.where(own_part <= position, 1.0, 0.0), axis=0, keepdims=True)
            slot = position - total_row + float(kept)
            pair_index = jnp.sum(jnp.where(pair_ends <= slot, 1.0, 0.0), axis=0, keepdims=True)
            column = jnp.where(position < total_row, own_index, float(place[1] * n_img) + pair_index)
            midx[k : k + 1, :] = jnp.where(lane < R, column, -1.0).astype(jnp.int32)

    def send_x(yr):
        if yr:
            copies.wait("y", yr)
        copies.send(("xp", yr), img_at(0, yr), img_at(1, yr), dev(1))
        copies.send(("xm", yr), img_at(0, yr), img_at(3, yr), dev(-1))

    def wait_image(xr, yr):
        if yr == 2 and xr != 2:
            for part in range(2):
                copies.wait(*(("g", xr, part) if xr else ("y2", 2 * part + 1)))
        elif xr or yr:
            copies.wait(("y", "xp", "xr", "xm")[xr], yr)

    def relay_x(yr):
        xr = 1 if yr % 2 == 0 else 3
        wait_image(xr, yr)
        copies.send(("xr", yr), img_at(xr, yr), img_at(2, yr), dev(sign(yr)))

    def relay_y(yr):
        copies.wait("y", yr)
        first, step = (0, -near) if yr == 1 else (half, near)
        copies.send(("y2", yr), img_at(0, yr, first, half), img_at(0, 2, first, half), dev(0, step))

    def across_y(xr, part):
        yr, first, step = ((3, 0, near), (1, half, -near))[part]
        wait_image(xr, yr)
        copies.send(("g", xr, part), img_at(xr, yr, first, half), img_at(xr, 2, first, half), dev(0, step))

    def tail(t):
        if t >= 2:
            make_tail(t)
        copies.send(("t", t), tsend.at[t], trecv.at[pl.ds(t * R, R)], partner)
        if t == YPOS - 1:
            copies.send(("y", 1), img_at(0, 0), img_at(0, 1), partner)
            copies.send(("y", 3), img_at(0, 0), img_at(0, 3), dev(0, -near))

    def pack(k):
        if k >= 2:
            block = normalize(cap_ref[pl.ds(k * R, R), :])[0]
            copies.wait("t", k - 2)
            count = (k - 1) * R
            row = (lax.broadcasted_iota(jnp.int32, (R, count), 0) + k * R).astype(F32)
            lane = lax.broadcasted_iota(jnp.int32, (R, count), 1).astype(F32)
            pick = jnp.where(row - tots[0:1, :count] == lane, 1.0, 0.0).astype(BF16)
            moved = jnp.dot(pick, trecv[pl.ds(0, count), :], preferred_element_type=F32)
            block = jnp.where(before_total(k * R), block, moved)
            capbuf[pl.ds(k * rows, R), :] = block.astype(BF16)
        copies.send(("zp", k), cap_at(k, 0, 0), cap_at(k, 0, 1), dev(0, 0, 1))
        copies.send(("zm", k), cap_at(k, 0, 0), cap_at(k, 0, 3), dev(0, 0, -1))
        copies.send(("s", 0, k), cap_at(k, 0, 0), cap_at(k, 1, 0), sibling)

    def forward(k, zr):
        copies.wait(("", "zp", "zr", "zm")[zr], k)
        if zr != 2 and (zr == 1) == (k % 2 == 0):
            copies.send(("zr", k), cap_at(k, 0, zr), cap_at(k, 0, 2), dev(0, 0, sign(k)))
        copies.send(("s", zr, k), cap_at(k, 0, zr), cap_at(k, 1, zr), sibling)

    def weights(k, xr):
        for zr in range(4):
            copies.wait("s", zr, k)
        for yr in range(4):
            wait_image(xr, yr)
        products = lax.dot_general(
            imgbuf[pl.ds(xr * cols, cols), :],
            capbuf[pl.ds(k * rows, rows), :],
            (((1,), (1,)), ((), ())),
            preferred_element_type=F32,
        )
        scale = consts[0:1, :]
        half_tanh = scale * jnp.tanh(products * scale + consts[1:2, :])
        if xr == 0:
            image = lax.broadcasted_iota(jnp.int32, (cols, rows), 0)
            half_tanh = half_tanh + jnp.where(image == midx[k : k + 1, :], -scale, scale)
        else:
            half_tanh = half_tanh + scale
        wt[pl.ds(xr * cols, cols), pl.ds(k * rows, rows)] = half_tanh.astype(BF16)

    def caption_part(k):
        def of(side):
            block = wt[:, pl.ds(k * rows + side * 4 * R, 4 * R)]
            return lax.dot_general(block, imgbuf[...], (((0,), (0,)), ((), ())), preferred_element_type=F32)

        d2ds[k] = of(1).astype(BF16)
        copies.send(("d", k), d2ds.at[k], d2dr.at[k], sibling)
        pown[k] = of(0)

    def z_first(k):
        copies.wait("d", k)
        step = sign(k)
        direct, late = (1, 3) if step == 1 else (3, 1)

        def total(zr):
            here = slice(zr * R, zr * R + R)
            return pown[k, here, :] + d2dr[k, here, :].astype(F32)

        zsrel[k] = total(2).astype(BF16)
        copies.send(("zrel", k), zsrel.at[k], zrrel.at[k], dev(0, 0, step))
        zsdir[k] = total(direct).astype(BF16)
        copies.send(("zdir", k), zsdir.at[k], zrdir.at[k], dev(0, 0, -step))
        pown[k, 0:R, :] = total(0)
        pown[k, late * R : late * R + R, :] = total(late)

    def z_late(k):
        copies.wait("zrel", k)
        step = sign(k)
        late = 3 if step == 1 else 1
        zsdep[k] = (pown[k, late * R : late * R + R, :] + zrrel[k].astype(F32)).astype(BF16)
        copies.send(("zdep", k), zsdep.at[k], zrdep.at[k], dev(0, 0, step))

    def project(first, sums, live):
        unit, inverse = normalize(cap_ref[pl.ds(first, R), :])
        grads = (sums - unit * jnp.sum(unit * sums, axis=1, keepdims=True)) * inverse
        cout[pl.ds(first, R), :] = jnp.where(live, grads, 0.0)

    def z_last(k):
        copies.wait("zdir", k)
        copies.wait("zdep", k)
        sums = pown[k, 0:R, :] + zrdir[k].astype(F32) + zrdep[k].astype(F32)
        gsb[pl.ds(k * R, R), :] = sums.astype(BF16)
        if k >= 2:
            t = k - 2
            count = kept - k * R
            row = lax.broadcasted_iota(jnp.int32, (R, count), 0).astype(F32)
            lane = (lax.broadcasted_iota(jnp.int32, (R, count), 1) + 2 * R).astype(F32)
            pick = jnp.where(row + tots[0:1, :count] == lane, 1.0, 0.0).astype(BF16)
            ts2[t] = jnp.dot(pick, gsb[pl.ds(k * R, count), :], preferred_element_type=F32).astype(BF16)
            copies.send(("tb", t), ts2.at[t], tr2.at[t], partner)
        live = before_total(k * R)
        project(k * R, jnp.where(live, sums, 0.0), live)

    def tail_last(t):
        copies.wait("tb", t)
        live = before_total(kept + t * R)
        project(kept + t * R, jnp.where(live, tr2[t].astype(F32), 0.0), live)

    def image_part(xr, h):
        first = xr * cols + h * two
        part = jnp.dot(wt[pl.ds(first, two), :], capbuf[...], preferred_element_type=F32)
        here = pl.ds(h * two, two)
        pairs = [(yr, pl.ds(place[yr] * n_img, n_img)) for yr in ((2, 0) if h == 0 else (1, 3))]
        if xr == 0:
            xown[here, :] = part
        elif xr == 2:
            xsrel[here, :] = part.astype(BF16)
            for yr, at in pairs:
                copies.send(("xrel", yr), xsrel.at[at], xrrel.at[at], dev(sign(yr)))
        elif (h == 0) == (xr == 3):
            xdep[here, :] = part
        else:
            xsdir[here, :] = part.astype(BF16)
            for yr, at in pairs:
                copies.send(("xdir", yr), xsdir.at[at], xrdir.at[at], dev(-sign(yr)))

    def x_late(yr):
        copies.wait("xrel", yr)
        here = pl.ds(place[yr] * n_img, n_img)
        xsdep[here, :] = (xdep[here, :] + xrrel[here, :].astype(F32)).astype(BF16)
        copies.send(("xdep", yr), xsdep.at[here], xrdep.at[here], dev(sign(yr)))

    low, high = pl.ds(0, half), pl.ds(half, half)

    def x_last(yr):
        copies.wait("xdir", yr)
        copies.wait("xdep", yr)
        here = pl.ds(place[yr] * n_img, n_img)
        sums = xown[here, :] + xrdir[here, :].astype(F32) + xrdep[here, :].astype(F32)
        if yr == 0:
            yown[...] = sums
        elif yr == 2:
            ysrel[...] = sums.astype(BF16)
            copies.send(("yrel", 0), ysrel.at[low], yrrel.at[low], partner)
            copies.send(("yrel", 1), ysrel.at[high], yrrel.at[high], dev(0, -near))
        elif yr == 1:
            ysdir[low, :] = sums[:half, :].astype(BF16)
            copies.send(("ydir", 1), ysdir.at[low], yrdir.at[low], partner)
            ydep[high, :] = sums[half:, :]
        else:
            ysdir[high, :] = sums[half:, :].astype(BF16)
            copies.send(("ydir", 3), ysdir.at[high], yrdir.at[high], dev(0, -near))
            ydep[low, :] = sums[:half, :]

    def y_late(part):
        copies.wait("yrel", part)
        here = (low, high)[part]
        ysdep[here, :] = (ydep[here, :] + yrrel[here, :].astype(F32)).astype(BF16)
        copies.send(("ydep", part), ysdep.at[here], yrdep.at[here], partner if part else dev(0, -near))

    def finish():
        for name in (("ydir", 1), ("ydir", 3), ("ydep", 0), ("ydep", 1)):
            copies.wait(*name)
        sums = yown[...] + yrdir[...].astype(F32) + yrdep[...].astype(F32)
        unit, inverse = normalize(img_ref[...])
        iout[...] = (sums - unit * jnp.sum(unit * sums, axis=1, keepdims=True)) * inverse

    actions = dict(
        sx=send_x, gy=across_y, rx=relay_x, ry=relay_y, t=tail, p=pack, f=forward, A=weights, B=caption_part, C=image_part,
        zf=z_first, zl=z_late, zz=z_last, e=tail_last, xl=x_late, xz=x_last, yz=y_late, end=finish,
    )
    for kind, *numbers in ORDER:
        if (kind, *numbers) == SETUP:
            setup()
        actions[kind](*numbers)
    copies.drain()


def shards(image_embed, caption_vectors, caption_counts, natural_log_multiplier, match_odds_offset):
    n_img, width = image_embed.shape
    n_slot = caption_vectors.shape[0]
    kept = 9 * n_img // 2
    nk, nt = kept // R, (n_slot - kept) // R
    cols, rows = 4 * n_img, 8 * R
    vmem = pl.BlockSpec(memory_space=pltpu.VMEM)
    smem = pl.BlockSpec(memory_space=pltpu.SMEM)
    anywhere = pl.BlockSpec(memory_space=pl.ANY)

    def buf(*shape, dtype=BF16):
        return pltpu.VMEM((*shape, width), dtype)

    scratch = [
        buf(n_img),
        buf(n_slot),
        pltpu.VMEM((caption_counts.shape[0] // (2 * n_img), 2 * n_img), jnp.int32),
        pltpu.SemaphoreType.DMA((3,)),
        buf(4 * cols),
        buf(nk * rows),
        buf(R),
        buf(nt, R),
        buf(nt * R),
        pltpu.VMEM((4 * cols, nk * rows), BF16),
        pltpu.VMEM((16, rows), jnp.int32),
        pltpu.VMEM((8, width), F32),
        pltpu.VMEM((8, rows), F32),
        buf(nk, 4 * R, dtype=F32),
        buf(nk, 4 * R),
        buf(nk, 4 * R),
        *[buf(nk, R)] * 6,
        buf(R, dtype=F32),
        buf(kept),
        buf(nt, R),
        buf(nt, R),
        *[buf(cols, dtype=F32)] * 2,
        *[buf(cols)] * 6,
        *[buf(n_img, dtype=F32)] * 2,
        *[buf(n_img)] * 6,
        pltpu.SemaphoreType.DMA((160,)),
        pltpu.SemaphoreType.DMA((160,)),
    ]
    return pl.pallas_call(
        kernel,
        out_shape=(
            pltpu.VMEM((n_img, width), F32),
            pltpu.VMEM((n_slot, width), F32),
        ),
        in_specs=[anywhere, anywhere, anywhere, smem, smem],
        out_specs=(vmem, vmem),
        scratch_shapes=scratch,
        compiler_params=pltpu.CompilerParams(
            collective_id=0, has_side_effects=True, vmem_limit_bytes=60 * 1024 * 1024
        ),
    )(image_embed, caption_vectors, caption_counts.reshape(-1, 2 * n_img), natural_log_multiplier, match_odds_offset)


def solution(mesh):
    placed = (P(("blk", "group"), None), P(("blk", "group"), None), P(), P(), P())
    return jax.shard_map(
        shards,
        mesh=mesh,
        in_specs=placed,
        out_specs=(P(("blk", "group"), None), P(("blk", "group"), None)),
        check_vma=False,
    )
```
